32 devices in a mesh: dp: 16 (over z, y, x), rep: 2 (over core).
Axes of the slice: x: 2, y: 2, z: 4, core: 2. Of those that a mesh axis runs over, the one named last changes fastest.
Arguments:
- tokens: bfloat16 [2, 1024, 4096], P('rep'), may hold values from -6 to 6
- cotangent: bfloat16 [2, 1024, 4096], P('rep'), may hold values from -6 to 6
- lengths: int32 [2, 2], P('rep'), may hold values from 1 to 512
- w_in: bfloat16 [4096, 2, 14336], P(None, None, 'dp'), may hold values from -0.09375 to 0.09375
- w_down: bfloat16 [14336, 4096], P('dp'), may hold values from -0.046875 to 0.046875
Outputs:
- d_tokens: float32 [2, 1024, 4096], P('rep', 'dp')
- weight_grads: float32 [4096, 3, 14336], P('rep', None, 'dp')
The draws below stay inside these ranges and needn't reach their ends.
All inputs are finite; a program needn't handle non-finite values.
Results may differ from the reference program's by a relative error of at most 0.0029.
Values sent between devices are 32-bit elements; how exact they have to be, the bound alone decides.
A program may use at most 256 MiB of HBM per device.

```python
import jax
import jax.numpy as jnp

D = 4096
HID = 14336
ROWS = 1024
SEQS = 2
SLOTS = 512
N_REP = 2


def with_ends(entries, rng, low, high):
    place = [jax.random.randint(jax.random.fold_in(rng, axis), (), 0, length) for axis, length in enumerate(entries.shape)]
    longest = entries.shape.index(max(entries.shape))
    beside = place[:longest] + [(place[longest] + 1) % entries.shape[longest]] + place[longest + 1:]
    return entries.at[tuple(place)].set(low).at[tuple(beside)].set(high)


def levels(rng, extent, cuts, low, largest):
    def one(dim, shards_of):
        draws = jax.random.uniform(jax.random.fold_in(jax.random.fold_in(rng, 6), dim), (shards_of,), jnp.float32, low / len(cuts), largest / len(cuts))
        return jnp.repeat(jnp.exp(draws), extent[dim] // shards_of).reshape((-1,) + (1,) * (len(extent) - dim - 1))

    loudness = one(*cuts[0])
    for cut in cuts[1:]:
        loudness = loudness * one(*cut)
    return loudness


def centred(stream_key, dims, scale, bound, cuts=(), kind=jnp.bfloat16):
    values = scale * jax.random.normal(stream_key, dims, jnp.float32)
    if cuts:
        values = values * levels(stream_key, dims, cuts, -0.22, 0.18)
    return jnp.clip(values, -bound, bound).astype(kind)


def setup_inputs(seed: int = 0) -> dict:
    key_list = jax.random.split(jax.random.key(seed), 6)
    return {
        "tokens": centred(key_list[0], (N_REP, ROWS, D), 1.0, 6.0, ((0, 2),)),
        "cotangent": centred(key_list[1], (N_REP, ROWS, D), 1.0, 6.0, ((0, 2),)),
        "lengths": with_ends(jax.random.randint(key_list[2], (N_REP, SEQS), 1, SLOTS + 1), jax.random.fold_in(key_list[2], 1), 1, SLOTS).astype(jnp.int32),
        "w_in": centred(key_list[3], (D, 2, HID), D ** -0.5, 0.09375, ((2, 16),)),
        "w_down": centred(key_list[4], (HID, D), HID ** -0.5, 0.046875, ((0, 16),)),
    }


GRAD_SCALE = 0.03125


def reference(tokens, cotangent, lengths, w_in, w_down):
    hidden_units = w_down.shape[0]
    slots = ROWS // SEQS
    position = jnp.arange(ROWS)
    w_flat = w_in.reshape(D, 2 * hidden_units)
    zero_value = jnp.zeros((), jnp.bfloat16)
    total = jnp.zeros((D, 3, hidden_units), jnp.float32)
    results = []
    for replica in range(N_REP):
        limit = lengths[replica][position // slots]
        is_alive = (position % slots) < limit
        live_x = jnp.where(is_alive[:, None], tokens[replica], zero_value)
        live_dy = jnp.where(is_alive[:, None], cotangent[replica], zero_value)
        gate_up = jnp.dot(live_x, w_flat, preferred_element_type=jnp.float32)
        gate = gate_up[:, :hidden_units]
        upward = gate_up[:, hidden_units:]
        sigmoid_gate = jax.nn.sigmoid(gate)
        activated = gate * sigmoid_gate
        hidden = (activated * upward).astype(jnp.bfloat16)
        d_hidden = jnp.dot(live_dy, w_down.T, preferred_element_type=jnp.float32)
        d_gate = d_hidden * upward * sigmoid_gate * (1.0 + gate * (1.0 - sigmoid_gate))
        d_up = d_hidden * activated
        d_in = jnp.concatenate([d_gate, d_up], axis=1).astype(jnp.bfloat16)
        results.append(jnp.dot(d_in, w_flat.T, preferred_element_type=jnp.float32))
        grad_in = jnp.dot(live_x.T, d_in, preferred_element_type=jnp.float32)
        grad_down = jnp.dot(live_dy.T, hidden, preferred_element_type=jnp.float32)
        combined = jnp.concatenate([grad_in.reshape(D, 2, hidden_units), grad_down[:, None, :]], axis=1)
        total = total + combined * GRAD_SCALE
    return jnp.stack(results), total
```

```python
import functools
import jax
import jax.numpy as jnp
from jax import lax
from jax.experimental import pallas as pl
from jax.experimental.pallas import tpu as pltpu

from jax.sharding import PartitionSpec as P

GRAD_SCALE = 0.03125
COPIES_PER_ORDER = 2
MESH = pl.DeviceIdType.MESH
LINE = 4
NY = 2
NX = 2
LANES = 128
PLANE_FIRST_STAGES = (0, 2, 4, 5, 6, 7)
LINE_FIRST_GAP = 2
LINE_FIRST_SHARE = 5


def add_blocks(dst, src, lead):
    count = 1
    for n in lead:
        count *= n

    def body(i, carry):
        idx = []
        for n in reversed(lead):
            idx.append(lax.rem(i, n))
            i = i // n
        idx = tuple(reversed(idx))
        dst[idx] = dst[idx] + src[idx]
        return carry

    if count == 1:
        dst[...] = dst[...] + src[...]
    else:
        lax.fori_loop(0, count, body, 0)


def exchange_kernel(
    dims, d_in, hidden, w_ref, x_ref, dy_ref, out_ref, g_in, g_down,
    pa, rs1, rs2, zr, zl, pb, br, bl, bx, by, wbuf, xbuf, tin, tdown,
    s1s, s1r, s2s, s2r, zrs, zrr, zls, zlr, brs, brr, bls, blr, bxs, bxr, bys, byr,
    wsem, xsem, tis, tir, tds, tdr,
):
    nz, n_pairs, n_line, share, d_tile, n_tiles = dims
    d = lax.axis_index("dp")
    rep = lax.axis_index("rep")
    z, y, x = d // (NY * NX), lax.rem(d // NX, NY), lax.rem(d, NX)
    px = d + 1 - 2 * x
    py = d + NX * (1 - 2 * y)
    up, down = d + NY * NX, d - NY * NX
    has_up, has_down = z < nz - 1, z > 0
    other = 1 - rep
    width = 2 * LANES
    rows = d_in.shape[0]
    m_tile = NY * NX * share
    part = n_tiles * d_tile

    barrier = pltpu.get_barrier_semaphore()
    for peer in (px, py):
        pl.semaphore_signal(barrier, inc=1, device_id=(peer, rep), device_id_type=MESH)
    pl.semaphore_signal(barrier, inc=1, device_id=(d, other), device_id_type=MESH)

    @pl.when(has_up)
    def _():
        pl.semaphore_signal(barrier, inc=1, device_id=(up, rep), device_id_type=MESH)

    @pl.when(has_down)
    def _():
        pl.semaphore_signal(barrier, inc=1, device_id=(down, rep), device_id_type=MESH)

    pl.semaphore_wait(barrier, 3 + has_up.astype(jnp.int32) + has_down.astype(jnp.int32))

    def remote(src, dst, ssem, rsem, dev, core=None):
        return pltpu.make_async_remote_copy(
            src_ref=src, dst_ref=dst, send_sem=ssem, recv_sem=rsem,
            device_id=(dev, rep if core is None else core), device_id_type=MESH,
        )

    def first_x(p):
        return remote(pa.at[p, 0, :, :, 1 - x], rs1.at[p, 0], s1s.at[p, 0], s1r.at[p, 0], px)

    def first_y(p):
        return remote(pa.at[p, 1, :, 1 - y], rs1.at[p, 1], s1s.at[p, 1], s1r.at[p, 1], py)

    def second_y(p):
        return remote(pa.at[p, 0, :, 1 - y, x], rs2.at[p, 0], s2s.at[p, 0], s2r.at[p, 0], py)

    def second_x(p):
        return remote(pa.at[p, 1, :, y, 1 - x], rs2.at[p, 1], s2s.at[p, 1], s2r.at[p, 1], px)

    def line_up(p, k):
        return remote(pa.at[p, :, k, y, x], zr.at[p, k], zrs.at[p, k], zrr.at[p, k], up)

    def line_down(p, k):
        return remote(pa.at[p, :, k, y, x], zl.at[p, k], zls.at[p, k], zlr.at[p, k], down)

    def b_up(b, k):
        return remote(pb.at[b, k], br.at[b, k], brs.at[b, k], brr.at[b, k], up)

    def b_down(b, k):
        return remote(pb.at[b, k], bl.at[b, k], bls.at[b, k], blr.at[b, k], down)

    def b_y(b):
        return remote(pb.at[b, z, 1 - y], by.at[b], bys.at[b], byr.at[b], py)

    def b_x(b):
        return remote(pb.at[b, z, y, 1 - x], bx.at[b], bxs.at[b], bxr.at[b], px)

    def w_copy(c):
        slot = lax.rem(c, 2)
        return pltpu.make_async_copy(w_ref.at[pl.ds(c * width, width)], wbuf.at[slot], wsem.at[slot])

    n_chunks = n_pairs + n_line
    w_copy(0).start()

    def product(c, store):
        w_copy(c).wait()

        @pl.when(c + 1 < n_chunks)
        def _():
            w_copy(c + 1).start()

        slot = lax.rem(c, 2)

        def body(k, carry):
            val = lax.dot_general(
                d_in[pl.ds(pl.multiple_of(k * m_tile, m_tile), m_tile), :], wbuf[slot],
                (((1,), (1,)), ((), ())), preferred_element_type=jnp.float32,
            )
            store(k, val)
            return carry

        lax.fori_loop(0, nz, body, 0)

    def store_pair(p):
        def store(k, val):
            val = val.reshape(NY, NX, share, width)
            pa[p, 0, k] = val[..., :LANES]
            pa[p, 1, k] = val[..., LANES:]
        return store

    def store_line(b):
        def store(k, val):
            pb[b, k] = val.reshape(NY, NX, share, width)
        return store

    def x_copy(i, src, s):
        off = pl.multiple_of(other * part + i * d_tile, d_tile)
        return pltpu.make_async_copy(src.at[:, pl.ds(off, d_tile)], xbuf.at[s], xsem.at[s])

    def tin_send(i):
        slot = lax.rem(i, 2)
        return remote(tin.at[slot], g_in.at[pl.ds(i * d_tile, d_tile)], tis.at[slot], tir.at[i], d, other)

    def tdown_send(i):
        slot = lax.rem(i, 2)
        return remote(tdown.at[slot], g_down.at[pl.ds(i * d_tile, d_tile)], tds.at[slot], tdr.at[i], d, other)

    def tile(i):
        x_copy(i, x_ref, 0).wait()
        x_copy(i, dy_ref, 1).wait()
        slot = lax.rem(i, 2)

        @pl.when(i >= 2)
        def _():
            tin_send(i - 2).wait_send()
            tdown_send(i - 2).wait_send()

        n_w = LANES
        lhs = xbuf[0].T

        def body(n, carry):
            cols = pl.ds(pl.multiple_of(n * width, width), width)
            tin[slot, :, cols] = jnp.dot(lhs, d_in[:, cols], preferred_element_type=jnp.float32)
            return carry

        lax.fori_loop(0, d_in.shape[1] // width, body, 0)
        lhs2 = xbuf[1].T
        tdown[slot] = jnp.dot(lhs2, hidden[...], preferred_element_type=jnp.float32)

        @pl.when(i + 1 < n_tiles)
        def _():
            x_copy(i + 1, x_ref, 0).start()
            x_copy(i + 1, dy_ref, 1).start()

        tin_send(i).start()
        tdown_send(i).start()

    x_copy(0, x_ref, 0).start()
    x_copy(0, dy_ref, 1).start()

    def a0(p):
        product(p + jnp.minimum(lax.div(p, LINE_FIRST_GAP) + 1, n_line), store_pair(p))
        first_x(p).start()
        first_y(p).start()

    def a1(p):
        first_x(p).wait_recv()
        add_blocks(pa.at[p, 0, :, 1 - y, x], rs1.at[p, 0, :, 1 - y], (nz,))
        second_y(p).start()
        first_y(p).wait_recv()
        add_blocks(pa.at[p, 1, :, y, 1 - x], rs1.at[p, 1, :, 1 - x], (nz,))
        second_x(p).start()
        add_blocks(pa.at[p, 0, :, y, x], rs1.at[p, 0, :, y], (nz,))
        add_blocks(pa.at[p, 1, :, y, x], rs1.at[p, 1, :, x], (nz,))

    def a2(p):
        second_y(p).wait_recv()
        add_blocks(pa.at[p, 0, :, y, x], rs2.at[p, 0], (nz,))
        second_x(p).wait_recv()
        add_blocks(pa.at[p, 1, :, y, x], rs2.at[p, 1], (nz,))
        hop_send(0, functools.partial(line_up, p), functools.partial(line_down, p), None, None)

    def hop_send(h, cup, cdown, add_up, add_down):
        @pl.when(z == h)
        def _():
            for k in range(nz - 1, h, -1):
                if h:
                    cup(k).wait_recv()
                    add_up(k)
                cup(k).start()

        @pl.when(z == nz - 1 - h)
        def _():
            for k in range(0, nz - 1 - h):
                if h:
                    cdown(k).wait_recv()
                    add_down(k)
                cdown(k).start()

    def a_hop(h):
        def go(p):
            hop_send(
                h, functools.partial(line_up, p), functools.partial(line_down, p),
                lambda k: add_blocks(pa.at[p, :, k, y, x], zr.at[p, k], (2,)),
                lambda k: add_blocks(pa.at[p, :, k, y, x], zl.at[p, k], (2,)),
            )
        return go

    def a_last(p):
        @pl.when(has_down)
        def _():
            line_up(p, z).wait_recv()
            add_blocks(pa.at[p, :, z, y, x], zr.at[p, z], (2,))

        @pl.when(has_up)
        def _():
            line_down(p, z).wait_recv()
            add_blocks(pa.at[p, :, z, y, x], zl.at[p, z], (2,))

        c = p + jnp.minimum(lax.div(p, LINE_FIRST_GAP) + 1, n_line)
        for u in range(2):
            cols = pl.ds(pl.multiple_of(c * width + u * LANES, LANES), LANES)
            out_ref[:, cols] = pa[p, u, z, y, x]

    def b_chunk(b):
        return b * (LINE_FIRST_GAP + 1)

    def b0(b):
        product(b_chunk(b), store_line(b))
        hop_send(0, functools.partial(b_up, b), functools.partial(b_down, b), None, None)

    def b_hop(h):
        def go(b):
            hop_send(
                h, functools.partial(b_up, b), functools.partial(b_down, b),
                lambda k: add_blocks(pb.at[b, k], br.at[b, k], (NY, NX)),
                lambda k: add_blocks(pb.at[b, k], bl.at[b, k], (NY, NX)),
            )
        return go

    def b_plane(b):
        @pl.when(has_down)
        def _():
            b_up(b, z).wait_recv()
            add_blocks(pb.at[b, z], br.at[b, z], (NY, NX))

        @pl.when(has_up)
        def _():
            b_down(b, z).wait_recv()
            add_blocks(pb.at[b, z], bl.at[b, z], (NY, NX))

        b_y(b).start()

    def b_second(b):
        b_y(b).wait_recv()
        add_blocks(pb.at[b, z, y], by.at[b], (NX,))
        b_x(b).start()

    def b_last(b):
        b_x(b).wait_recv()
        cols = pl.ds(pl.multiple_of(b_chunk(b) * width, width), width)
        out_ref[:, cols] = pb[b, z, y, x] + bx[b]

    hops = nz - 1
    a_stages = [a0, a1, a2] + [a_hop(h) for h in range(1, hops)] + [a_last]
    b_stages = [b0] + [b_hop(h) for h in range(1, hops)] + [b_plane, b_second, b_last]
    a_at = PLANE_FIRST_STAGES
    b_at = [2 * j for j in range(len(b_stages))]
    n_steps = max(n_pairs + a_at[-1], (n_line - 1) * LINE_FIRST_GAP + b_at[-1] + 1, n_tiles)

    def step(t, carry):
        def run_b(j):
            s = t - b_at[j]

            @pl.when((s >= 0) & (lax.rem(s, LINE_FIRST_GAP) == 0) & (lax.div(s, LINE_FIRST_GAP) < n_line))
            def _():
                b_stages[j](lax.div(s, LINE_FIRST_GAP))

        def run_a(j):
            s = t - a_at[j]

            @pl.when((s >= 0) & (s < n_pairs))
            def _():
                a_stages[j](s)

        run_b(0)
        run_a(0)

        @pl.when(t < n_tiles)
        def _():
            tile(t)

        for j in range(1, len(a_stages)):
            run_a(j)
        for j in range(1, len(b_stages)):
            run_b(j)
        return carry

    lax.fori_loop(0, n_steps, step, 0)

    def drain(p, carry):
        for c in (first_x, first_y, second_y, second_x):
            c(p).wait_send()
        for k in range(nz):
            @pl.when(k > z)
            def _():
                line_up(p, k).wait_send()

            @pl.when(k < z)
            def _():
                line_down(p, k).wait_send()
        return carry

    lax.fori_loop(0, n_pairs, drain, 0)

    def drain_b(b, carry):
        b_y(b).wait_send()
        b_x(b).wait_send()
        for k in range(nz):
            @pl.when(k > z)
            def _():
                b_up(b, k).wait_send()

            @pl.when(k < z)
            def _():
                b_down(b, k).wait_send()
        return carry

    lax.fori_loop(0, n_line, drain_b, 0)
    for i in range(max(n_tiles - 2, 0), n_tiles):
        tin_send(i).wait_send()
        tdown_send(i).wait_send()

    def drain_t(i, carry):
        tin_send(i).wait_recv()
        tdown_send(i).wait_recv()
        return carry

    lax.fori_loop(0, n_tiles, drain_t, 0)


def exchange(d_in, hidden, w_flat, x_all, dy_all, n_dp, n_rep):
    rows, two_h = d_in.shape
    width = w_flat.shape[0]
    nz = n_dp // (NY * NX)
    share = rows // n_dp
    n_chunks = width // (2 * LANES)
    n_line = n_chunks // LINE_FIRST_SHARE
    n_pairs = n_chunks - n_line
    part = width // n_rep
    d_tile = 256
    n_tiles = part // d_tile
    dims = (nz, n_pairs, n_line, share, d_tile, n_tiles)
    f32 = jnp.float32
    dma = pltpu.SemaphoreType.DMA
    wide = 2 * LANES
    return pl.pallas_call(
        functools.partial(exchange_kernel, dims),
        out_shape=(
            jax.ShapeDtypeStruct((share, width), f32),
            jax.ShapeDtypeStruct((part, two_h), f32),
            jax.ShapeDtypeStruct((part, two_h // 2), f32),
        ),
        in_specs=[pl.BlockSpec(memory_space=pltpu.VMEM)] * 2 + [pl.BlockSpec(memory_space=pl.ANY)] * 3,
        out_specs=(
            pl.BlockSpec(memory_space=pltpu.VMEM),
            pl.BlockSpec(memory_space=pl.ANY),
            pl.BlockSpec(memory_space=pl.ANY),
        ),
        scratch_shapes=[
            pltpu.VMEM((n_pairs, 2, nz, NY, NX, share, LANES), f32),
            pltpu.VMEM((n_pairs, 2, nz, 2, share, LANES), f32),
            pltpu.VMEM((n_pairs, 2, nz, share, LANES), f32),
            pltpu.VMEM((n_pairs, nz, 2, share, LANES), f32),
            pltpu.VMEM((n_pairs, nz, 2, share, LANES), f32),
            pltpu.VMEM((n_line, nz, NY, NX, share, wide), f32),
            pltpu.VMEM((n_line, nz, NY, NX, share, wide), f32),
            pltpu.VMEM((n_line, nz, NY, NX, share, wide), f32),
            pltpu.VMEM((n_line, share, wide), f32),
            pltpu.VMEM((n_line, NX, share, wide), f32),
            pltpu.VMEM((2, wide, two_h), jnp.bfloat16),
            pltpu.VMEM((2, rows, d_tile), jnp.bfloat16),
            pltpu.VMEM((2, d_tile, two_h), f32),
            pltpu.VMEM((2, d_tile, two_h // 2), f32),
            dma((n_pairs, 2)), dma((n_pairs, 2)), dma((n_pairs, 2)), dma((n_pairs, 2)),
            dma((n_pairs, nz)), dma((n_pairs, nz)), dma((n_pairs, nz)), dma((n_pairs, nz)),
            dma((n_line, nz)), dma((n_line, nz)), dma((n_line, nz)), dma((n_line, nz)),
            dma((n_line,)), dma((n_line,)), dma((n_line,)), dma((n_line,)),
            dma((2,)), dma((2,)), dma((2,)), dma((n_tiles,)), dma((2,)), dma((n_tiles,)),
        ],
        compiler_params=pltpu.CompilerParams(
            collective_id=0, has_side_effects=True, vmem_limit_bytes=62 * 2**20
        ),
        cost_estimate=pl.CostEstimate(
            flops=5 * rows * width * two_h // 2, bytes_accessed=8 * width * two_h, transcendentals=0
        ),
    )(d_in, hidden, w_flat, x_all, dy_all)


def cube_code(index, bits):
    if bits < 2:
        return index
    return index ^ ((index >> 1) & (1 << (bits - 2)))


def bit_slice(blocks, axis, value):
    return lax.index_in_dim(blocks, value, axis, keepdims=False)


def copy_block(owners_ref, src_ref, dst_ref):
    dst_ref[...] = src_ref[...]


def reorder(owners, d_in, share):
    n_dp = owners.shape[0]
    width = d_in.shape[1]
    return pl.pallas_call(
        copy_block,
        out_shape=jax.ShapeDtypeStruct(d_in.shape, d_in.dtype),
        grid_spec=pltpu.PrefetchScalarGridSpec(
            num_scalar_prefetch=1,
            grid=(n_dp,),
            in_specs=[pl.BlockSpec((share, width), lambda i, owners: (owners[i], 0))],
            out_specs=pl.BlockSpec((share, width), lambda i, owners: (i, 0)),
        ),
        cost_estimate=pl.CostEstimate(
            flops=0, bytes_accessed=4 * d_in.size, transcendentals=0
        ),
        compiler_params=pltpu.CompilerParams(vmem_limit_bytes=8 * 2**20),
    )(owners, d_in)


def by_permutes(n_dp, n_rep, tokens, cotangent, lengths, w_in, w_down):
    rows = tokens.shape[1]
    width = tokens.shape[2]
    seqs = lengths.shape[1]
    slots = rows // seqs
    hidden_units = w_down.shape[0]
    bits = n_dp.bit_length() - 1
    share = rows // n_dp
    position = jnp.arange(rows)
    owner_seq = (position // slots)[:, None] == jnp.arange(seqs)[None, :]
    limit = jnp.sum(jnp.where(owner_seq, lengths[0][None, :], 0), axis=1)
    is_alive = position % slots < limit
    zero_value = jnp.zeros((), jnp.bfloat16)
    live_x = jnp.where(is_alive[:, None], tokens[0], zero_value)
    live_dy = jnp.where(is_alive[:, None], cotangent[0], zero_value)
    w_flat = lax.optimization_barrier(w_in.reshape(width, 2 * hidden_units))
    gate_up = jnp.dot(live_x, w_flat, preferred_element_type=jnp.float32)
    gate = gate_up[:, :hidden_units]
    upward = gate_up[:, hidden_units:]
    sigmoid_gate = jax.nn.sigmoid(gate)
    activated = gate * sigmoid_gate
    hidden = (activated * upward).astype(jnp.bfloat16)
    d_hidden = lax.dot_general(
        live_dy, w_down, (((1,), (1,)), ((), ())), preferred_element_type=jnp.float32
    )
    d_gate = d_hidden * upward * sigmoid_gate * (1.0 + gate * (1.0 - sigmoid_gate))
    d_up = d_hidden * activated
    d_in = jnp.concatenate([d_gate, d_up], axis=1).astype(jnp.bfloat16)

    me = lax.axis_index("dp")
    my_code = cube_code(me, bits)
    owners = cube_code(my_code ^ jnp.arange(n_dp, dtype=jnp.int32), bits)
    blocks = reorder(owners, d_in, share)
    blocks = blocks.reshape((2,) * bits + (share, 2 * hidden_units))

    n_chunks = bits * COPIES_PER_ORDER
    while width % n_chunks:
        n_chunks -= 1
    columns = width // n_chunks
    flows = []
    for chunk in range(n_chunks):
        order = [(chunk + step) % bits for step in range(bits)]
        weights = lax.slice_in_dim(w_flat, chunk * columns, (chunk + 1) * columns, axis=0)

        def product(part, weights=weights):
            return lax.dot_general(
                part, weights, (((part.ndim - 1,), (1,)), ((), ())), preferred_element_type=jnp.float32
            )

        axis = bits - 1 - order[0]
        sent = product(bit_slice(blocks, axis, 1))
        kept = product(bit_slice(blocks, axis, 0))
        flows.append((order, sent, kept))

    def partner_pairs(bit):
        return [(d, cube_code(cube_code(d, bits) ^ (1 << bit), bits)) for d in range(n_dp)]

    part = width // n_rep
    rep = lax.axis_index("rep")

    def gradients(owner, after):
        x_all, dy_all, d_all, h_all, _ = lax.optimization_barrier((live_x, live_dy, d_in, hidden, after))
        x_part = lax.dynamic_slice_in_dim(x_all, owner * part, part, 1)
        dy_part = lax.dynamic_slice_in_dim(dy_all, owner * part, part, 1)
        pairs = (
            (x_part, d_all[:, :hidden_units]),
            (x_part, d_all[:, hidden_units:]),
            (dy_part, h_all),
        )
        return lax.optimization_barrier(
            tuple(
                lax.dot_general(
                    rows_of, units, (((0,), (0,)), ((), ())), preferred_element_type=jnp.float32
                )
                for rows_of, units in pairs
            )
        )

    first_sent = tuple(sent for _, sent, _ in flows)
    totals = [[], [], []]
    for shift in range(1, n_rep):
        ring = [(r, (r + shift) % n_rep) for r in range(n_rep)]
        for kind, grad in enumerate(gradients((rep + shift) % n_rep, first_sent)):
            totals[kind].append(lax.ppermute(grad, "rep", ring))

    results = [None] * n_chunks
    state = {}
    for chunk, (order, sent, kept) in enumerate(flows):
        state[chunk] = (sent, kept, sorted(order, reverse=True))
    shared = None
    for step in range(bits):
        if step == 1:
            own = gradients(rep, tuple(state[chunk][0] for chunk in range(min(bits, n_chunks))))
            for kind in range(3):
                totals[kind].append(own[kind])
            shared = jnp.stack([sum(terms[1:], terms[0]) for terms in totals], axis=1) * GRAD_SCALE
        for chunk in range(n_chunks):
            order = flows[chunk][0]
            sent, kept, left = state[chunk]
            if step == bits - 1 and shared is not None and chunk >= n_chunks // 2:
                sent, _ = lax.optimization_barrier((sent, shared))
            got = lax.ppermute(sent, "dp", partner_pairs(order[step]))
            left = [b for b in left if b != order[step]]
            if step == bits - 1:
                results[chunk] = kept + got
            else:
                axis = left.index(order[step + 1])
                sent = bit_slice(kept, axis, 1) + bit_slice(got, axis, 1)
                kept = bit_slice(kept, axis, 0) + bit_slice(got, axis, 0)
                state[chunk] = (sent, kept, left)
    shard = jnp.concatenate(results, axis=1)
    return (shard[None], shared)


def by_kernels(n_dp, n_rep, tokens, cotangent, lengths, w_in, w_down):
    rows = tokens.shape[1]
    width = tokens.shape[2]
    seqs = lengths.shape[1]
    slots = rows // seqs
    hidden_units = w_down.shape[0]
    position = jnp.arange(rows)
    owner_seq = (position // slots)[:, None] == jnp.arange(seqs)[None, :]
    limit = jnp.sum(jnp.where(owner_seq, lengths[0][None, :], 0), axis=1)
    is_alive = (position % slots < limit)[:, None]
    w_flat = lax.optimization_barrier(w_in.reshape(width, 2 * hidden_units))
    gate_up = jnp.dot(tokens[0], w_flat, preferred_element_type=jnp.float32)
    gate = gate_up[:, :hidden_units]
    upward = gate_up[:, hidden_units:]
    sigmoid_gate = jax.nn.sigmoid(gate)
    activated = gate * sigmoid_gate
    hidden = jnp.where(is_alive, activated * upward, 0.0).astype(jnp.bfloat16)
    d_hidden = lax.dot_general(
        cotangent[0], w_down, (((1,), (1,)), ((), ())), preferred_element_type=jnp.float32
    )
    d_hidden = jnp.where(is_alive, d_hidden, 0.0)
    d_gate = d_hidden * upward * sigmoid_gate * (1.0 + gate * (1.0 - sigmoid_gate))
    d_up = d_hidden * activated
    d_in = jnp.concatenate([d_gate, d_up], axis=1).astype(jnp.bfloat16)

    shard, got_in, got_down = exchange(d_in, hidden, w_flat, tokens[0], cotangent[0], n_dp, n_rep)
    part = width // n_rep
    start = lax.axis_index("rep") * part
    x_part = lax.dynamic_slice_in_dim(tokens[0], start, part, 1)
    dy_part = lax.dynamic_slice_in_dim(cotangent[0], start, part, 1)

    def own(rows_of, units):
        return lax.dot_general(rows_of, units, (((0,), (0,)), ((), ())), preferred_element_type=jnp.float32)

    own_in = own(x_part, d_in) + got_in
    own_down = own(dy_part, hidden) + got_down
    total = jnp.stack([own_in[:, :hidden_units], own_in[:, hidden_units:], own_down], axis=1)
    return (shard[None], total * GRAD_SCALE)


def fits_kernels(n_dp, n_rep, rows, width, hidden_units):
    return (
        n_rep == 2
        and n_dp == LINE * NY * NX
        and rows % (8 * n_dp) == 0
        and width % (n_rep * 256) == 0
        and hidden_units % (2 * LANES) in (0, LANES)
    )


def solution(mesh):
    n_dp = mesh.shape["dp"]
    n_rep = mesh.shape["rep"]

    def body(*args):
        tokens, _, _, _, w_down = args
        fast = fits_kernels(n_dp, n_rep, tokens.shape[1], tokens.shape[2], w_down.shape[0])
        return (by_kernels if fast else by_permutes)(n_dp, n_rep, *args)

    in_specs = (
        P("rep", None, None),
        P("rep", None, None),
        P("rep", None),
        P(None, None, "dp"),
        P("dp", None),
    )
    out_specs = (P("rep", "dp", None), P("rep", None, "dp"))
    return jax.shard_map(
        body, mesh=mesh, in_specs=in_specs, out_specs=out_specs, check_vma=False
    )
```

```python
import functools
import jax
import jax.numpy as jnp
from jax import lax
from jax.experimental import pallas as pl
from jax.experimental.pallas import tpu as pltpu

from jax.sharding import PartitionSpec as P

GRAD_SCALE = 0.03125
COPIES_PER_ORDER = 2
MESH = pl.DeviceIdType.MESH
LINE = 4
NY = 2
NX = 2
LANES = 128
PLANE_FIRST_STAGES = (0, 3, 6, 8, 10, 12)
LINE_FIRST_GAP = 2
LINE_FIRST_SHARE = 4


def add_blocks(dst, src, lead):
    count = 1
    for n in lead:
        count *= n

    def body(i, carry):
        idx = []
        for n in reversed(lead):
            idx.append(lax.rem(i, n))
            i = i // n
        idx = tuple(reversed(idx))
        dst[idx] = dst[idx] + src[idx]
        return carry

    if count == 1:
        dst[...] = dst[...] + src[...]
    else:
        lax.fori_loop(0, count, body, 0)


def exchange_kernel(
    dims, d_in, hidden, w_ref, x_ref, dy_ref, out_ref, g_in, g_down,
    pa, rs1, rs2, zr, zl, pb, br, bl, bx, by, wbuf, xbuf, tin, tdown,
    s1s, s1r, s2s, s2r, zrs, zrr, zls, zlr, brs, brr, bls, blr, bxs, bxr, bys, byr,
    wsem, xsem, tis, tir, tds, tdr,
):
    nz, n_pairs, n_line, share, d_tile, n_tiles = dims
    d = lax.axis_index("dp")
    rep = lax.axis_index("rep")
    z, y, x = d // (NY * NX), lax.rem(d // NX, NY), lax.rem(d, NX)
    px = d + 1 - 2 * x
    py = d + NX * (1 - 2 * y)
    up, down = d + NY * NX, d - NY * NX
    has_up, has_down = z < nz - 1, z > 0
    other = 1 - rep
    width = 2 * LANES
    rows = d_in.shape[0]
    m_tile = NY * NX * share
    part = n_tiles * d_tile

    barrier = pltpu.get_barrier_semaphore()
    for peer in (px, py):
        pl.semaphore_signal(barrier, inc=1, device_id=(peer, rep), device_id_type=MESH)
    pl.semaphore_signal(barrier, inc=1, device_id=(d, other), device_id_type=MESH)

    @pl.when(has_up)
    def _():
        pl.semaphore_signal(barrier, inc=1, device_id=(up, rep), device_id_type=MESH)

    @pl.when(has_down)
    def _():
        pl.semaphore_signal(barrier, inc=1, device_id=(down, rep), device_id_type=MESH)

    pl.semaphore_wait(barrier, 3 + has_up.astype(jnp.int32) + has_down.astype(jnp.int32))

    def remote(src, dst, ssem, rsem, dev, core=None):
        return pltpu.make_async_remote_copy(
            src_ref=src, dst_ref=dst, send_sem=ssem, recv_sem=rsem,
            device_id=(dev, rep if core is None else core), device_id_type=MESH,
        )

    def first_x(p):
        return remote(pa.at[p, 0, :, :, 1 - x], rs1.at[p, 0], s1s.at[p, 0], s1r.at[p, 0], px)

    def first_y(p):
        return remote(pa.at[p, 1, :, 1 - y], rs1.at[p, 1], s1s.at[p, 1], s1r.at[p, 1], py)

    def second_y(p):
        return remote(pa.at[p, 0, :, 1 - y, x], rs2.at[p, 0], s2s.at[p, 0], s2r.at[p, 0], py)

    def second_x(p):
        return remote(pa.at[p, 1, :, y, 1 - x], rs2.at[p, 1], s2s.at[p, 1], s2r.at[p, 1], px)

    def line_up(p, k):
        return remote(pa.at[p, :, k, y, x], zr.at[p, k], zrs.at[p, k], zrr.at[p, k], up)

    def line_down(p, k):
        return remote(pa.at[p, :, k, y, x], zl.at[p, k], zls.at[p, k], zlr.at[p, k], down)

    def b_up(b, k):
        return remote(pb.at[b, k], br.at[b, k], brs.at[b, k], brr.at[b, k], up)

    def b_down(b, k):
        return remote(pb.at[b, k], bl.at[b, k], bls.at[b, k], blr.at[b, k], down)

    def b_y(b):
        return remote(pb.at[b, z, 1 - y], by.at[b], bys.at[b], byr.at[b], py)

    def b_x(b):
        return remote(pb.at[b, z, y, 1 - x], bx.at[b], bxs.at[b], bxr.at[b], px)

    def w_copy(c):
        slot = lax.rem(c, 2)
        return pltpu.make_async_copy(w_ref.at[pl.ds(c * width, width)], wbuf.at[slot], wsem.at[slot])

    n_chunks = n_pairs + n_line
    w_copy(0).start()

    def product(c, store):
        w_copy(c).wait()

        @pl.when(c + 1 < n_chunks)
        def _():
            w_copy(c + 1).start()

        slot = lax.rem(c, 2)

        def body(k, carry):
            val = lax.dot_general(
                d_in[pl.ds(pl.multiple_of(k * m_tile, m_tile), m_tile), :], wbuf[slot],
                (((1,), (1,)), ((), ())), preferred_element_type=jnp.float32,
            )
            store(k, val)
            return carry

        lax.fori_loop(0, nz, body, 0)

    def store_pair(p):
        def store(k, val):
            val = val.reshape(NY, NX, share, width)
            pa[p, 0, k] = val[..., :LANES]
            pa[p, 1, k] = val[..., LANES:]
        return store

    def store_line(b):
        def store(k, val):
            pb[b, k] = val.reshape(NY, NX, share, width)
        return store

    def x_copy(i, src, s):
        off = pl.multiple_of(other * part + i * d_tile, d_tile)
        return pltpu.make_async_copy(src.at[:, pl.ds(off, d_tile)], xbuf.at[s], xsem.at[s])

    def tin_send(i):
        slot = lax.rem(i, 2)
        return remote(tin.at[slot], g_in.at[pl.ds(i * d_tile, d_tile)], tis.at[slot], tir.at[i], d, other)

    def tdown_send(i):
        slot = lax.rem(i, 2)
        return remote(tdown.at[slot], g_down.at[pl.ds(i * d_tile, d_tile)], tds.at[slot], tdr.at[i], d, other)

    def tile(i):
        x_copy(i, x_ref, 0).wait()
        x_copy(i, dy_ref, 1).wait()
        slot = lax.rem(i, 2)

        @pl.when(i >= 2)
        def _():
            tin_send(i - 2).wait_send()
            tdown_send(i - 2).wait_send()

        n_w = LANES
        lhs = xbuf[0].T

        def body(n, carry):
            cols = pl.ds(pl.multiple_of(n * width, width), width)
            tin[slot, :, cols] = jnp.dot(lhs, d_in[:, cols], preferred_element_type=jnp.float32)
            return carry

        lax.fori_loop(0, d_in.shape[1] // width, body, 0)
        lhs2 = xbuf[1].T
        tdown[slot] = jnp.dot(lhs2, hidden[...], preferred_element_type=jnp.float32)

        @pl.when(i + 1 < n_tiles)
        def _():
            x_copy(i + 1, x_ref, 0).start()
            x_copy(i + 1, dy_ref, 1).start()

        tin_send(i).start()
        tdown_send(i).start()

    x_copy(0, x_ref, 0).start()
    x_copy(0, dy_ref, 1).start()

    def a0(p):
        product(p + jnp.minimum(lax.div(p, LINE_FIRST_GAP) + 1, n_line), store_pair(p))
        first_x(p).start()
        first_y(p).start()

    def a1(p):
        first_x(p).wait_recv()
        add_blocks(pa.at[p, 0, :, 1 - y, x], rs1.at[p, 0, :, 1 - y], (nz,))
        second_y(p).start()
        first_y(p).wait_recv()
        add_blocks(pa.at[p, 1, :, y, 1 - x], rs1.at[p, 1, :, 1 - x], (nz,))
        second_x(p).start()
        add_blocks(pa.at[p, 0, :, y, x], rs1.at[p, 0, :, y], (nz,))
        add_blocks(pa.at[p, 1, :, y, x], rs1.at[p, 1, :, x], (nz,))

    def a2(p):
        second_y(p).wait_recv()
        add_blocks(pa.at[p, 0, :, y, x], rs2.at[p, 0], (nz,))
        second_x(p).wait_recv()
        add_blocks(pa.at[p, 1, :, y, x], rs2.at[p, 1], (nz,))
        hop_send(0, functools.partial(line_up, p), functools.partial(line_down, p), None, None)

    def hop_send(h, cup, cdown, add_up, add_down):
        @pl.when(z == h)
        def _():
            for k in range(nz - 1, h, -1):
                if h:
                    cup(k).wait_recv()
                    add_up(k)
                cup(k).start()

        @pl.when(z == nz - 1 - h)
        def _():
            for k in range(0, nz - 1 - h):
                if h:
                    cdown(k).wait_recv()
                    add_down(k)
                cdown(k).start()

    def a_hop(h):
        def go(p):
            hop_send(
                h, functools.partial(line_up, p), functools.partial(line_down, p),
                lambda k: add_blocks(pa.at[p, :, k, y, x], zr.at[p, k], (2,)),
                lambda k: add_blocks(pa.at[p, :, k, y, x], zl.at[p, k], (2,)),
            )
        return go

    def a_last(p):
        @pl.when(has_down)
        def _():
            line_up(p, z).wait_recv()
            add_blocks(pa.at[p, :, z, y, x], zr.at[p, z], (2,))

        @pl.when(has_up)
        def _():
            line_down(p, z).wait_recv()
            add_blocks(pa.at[p, :, z, y, x], zl.at[p, z], (2,))

        c = p + jnp.minimum(lax.div(p, LINE_FIRST_GAP) + 1, n_line)
        for u in range(2):
            cols = pl.ds(pl.multiple_of(c * width + u * LANES, LANES), LANES)
            out_ref[:, cols] = pa[p, u, z, y, x]

    def b_chunk(b):
        return b * (LINE_FIRST_GAP + 1)

    def b0(b):
        product(b_chunk(b), store_line(b))
        hop_send(0, functools.partial(b_up, b), functools.partial(b_down, b), None, None)

    def b_hop(h):
        def go(b):
            hop_send(
                h, functools.partial(b_up, b), functools.partial(b_down, b),
                lambda k: add_blocks(pb.at[b, k], br.at[b, k], (NY, NX)),
                lambda k: add_blocks(pb.at[b, k], bl.at[b, k], (NY, NX)),
            )
        return go

    def b_plane(b):
        @pl.when(has_down)
        def _():
            b_up(b, z).wait_recv()
            add_blocks(pb.at[b, z], br.at[b, z], (NY, NX))

        @pl.when(has_up)
        def _():
            b_down(b, z).wait_recv()
            add_blocks(pb.at[b, z], bl.at[b, z], (NY, NX))

        b_y(b).start()

    def b_second(b):
        b_y(b).wait_recv()
        add_blocks(pb.at[b, z, y], by.at[b], (NX,))
        b_x(b).start()

    def b_last(b):
        b_x(b).wait_recv()
        cols = pl.ds(pl.multiple_of(b_chunk(b) * width, width), width)
        out_ref[:, cols] = pb[b, z, y, x] + bx[b]

    hops = nz - 1
    a_stages = [a0, a1, a2] + [a_hop(h) for h in range(1, hops)] + [a_last]
    b_stages = [b0] + [b_hop(h) for h in range(1, hops)] + [b_plane, b_second, b_last]
    a_at = PLANE_FIRST_STAGES
    b_at = [2 * j for j in range(len(b_stages))]
    n_steps = max(n_pairs + a_at[-1], (n_line - 1) * LINE_FIRST_GAP + b_at[-1] + 1, n_tiles)

    def step(t, carry):
        def run_b(j):
            s = t - b_at[j]

            @pl.when((s >= 0) & (lax.rem(s, LINE_FIRST_GAP) == 0) & (lax.div(s, LINE_FIRST_GAP) < n_line))
            def _():
                b_stages[j](lax.div(s, LINE_FIRST_GAP))

        def run_a(j):
            s = t - a_at[j]

            @pl.when((s >= 0) & (s < n_pairs))
            def _():
                a_stages[j](s)

        run_b(0)
        run_a(0)

        @pl.when(t < n_tiles)
        def _():
            tile(t)

        for j in range(1, len(a_stages)):
            run_a(j)
        for j in range(1, len(b_stages)):
            run_b(j)
        return carry

    lax.fori_loop(0, n_steps, step, 0)

    def drain(p, carry):
        for c in (first_x, first_y, second_y, second_x):
            c(p).wait_send()
        for k in range(nz):
            @pl.when(k > z)
            def _():
                line_up(p, k).wait_send()

            @pl.when(k < z)
            def _():
                line_down(p, k).wait_send()
        return carry

    lax.fori_loop(0, n_pairs, drain, 0)

    def drain_b(b, carry):
        b_y(b).wait_send()
        b_x(b).wait_send()
        for k in range(nz):
            @pl.when(k > z)
            def _():
                b_up(b, k).wait_send()

            @pl.when(k < z)
            def _():
                b_down(b, k).wait_send()
        return carry

    lax.fori_loop(0, n_line, drain_b, 0)
    for i in range(max(n_tiles - 2, 0), n_tiles):
        tin_send(i).wait_send()
        tdown_send(i).wait_send()

    def drain_t(i, carry):
        tin_send(i).wait_recv()
        tdown_send(i).wait_recv()
        return carry

    lax.fori_loop(0, n_tiles, drain_t, 0)


def exchange(d_in, hidden, w_flat, x_all, dy_all, n_dp, n_rep):
    rows, two_h = d_in.shape
    width = w_flat.shape[0]
    nz = n_dp // (NY * NX)
    share = rows // n_dp
    n_chunks = width // (2 * LANES)
    n_line = n_chunks // LINE_FIRST_SHARE
    n_pairs = n_chunks - n_line
    part = width // n_rep
    d_tile = 256
    n_tiles = part // d_tile
    dims = (nz, n_pairs, n_line, share, d_tile, n_tiles)
    f32 = jnp.float32
    dma = pltpu.SemaphoreType.DMA
    wide = 2 * LANES
    return pl.pallas_call(
        functools.partial(exchange_kernel, dims),
        out_shape=(
            jax.ShapeDtypeStruct((share, width), f32),
            jax.ShapeDtypeStruct((part, two_h), f32),
            jax.ShapeDtypeStruct((part, two_h // 2), f32),
        ),
        in_specs=[pl.BlockSpec(memory_space=pltpu.VMEM)] * 2 + [pl.BlockSpec(memory_space=pl.ANY)] * 3,
        out_specs=(
            pl.BlockSpec(memory_space=pltpu.VMEM),
            pl.BlockSpec(memory_space=pl.ANY),
            pl.BlockSpec(memory_space=pl.ANY),
        ),
        scratch_shapes=[
            pltpu.VMEM((n_pairs, 2, nz, NY, NX, share, LANES), f32),
            pltpu.VMEM((n_pairs, 2, nz, 2, share, LANES), f32),
            pltpu.VMEM((n_pairs, 2, nz, share, LANES), f32),
            pltpu.VMEM((n_pairs, nz, 2, share, LANES), f32),
            pltpu.VMEM((n_pairs, nz, 2, share, LANES), f32),
            pltpu.VMEM((n_line, nz, NY, NX, share, wide), f32),
            pltpu.VMEM((n_line, nz, NY, NX, share, wide), f32),
            pltpu.VMEM((n_line, nz, NY, NX, share, wide), f32),
            pltpu.VMEM((n_line, share, wide), f32),
            pltpu.VMEM((n_line, NX, share, wide), f32),
            pltpu.VMEM((2, wide, two_h), jnp.bfloat16),
            pltpu.VMEM((2, rows, d_tile), jnp.bfloat16),
            pltpu.VMEM((2, d_tile, two_h), f32),
            pltpu.VMEM((2, d_tile, two_h // 2), f32),
            dma((n_pairs, 2)), dma((n_pairs, 2)), dma((n_pairs, 2)), dma((n_pairs, 2)),
            dma((n_pairs, nz)), dma((n_pairs, nz)), dma((n_pairs, nz)), dma((n_pairs, nz)),
            dma((n_line, nz)), dma((n_line, nz)), dma((n_line, nz)), dma((n_line, nz)),
            dma((n_line,)), dma((n_line,)), dma((n_line,)), dma((n_line,)),
            dma((2,)), dma((2,)), dma((2,)), dma((n_tiles,)), dma((2,)), dma((n_tiles,)),
        ],
        compiler_params=pltpu.CompilerParams(
            collective_id=0, has_side_effects=True, vmem_limit_bytes=62 * 2**20
        ),
        cost_estimate=pl.CostEstimate(
            flops=5 * rows * width * two_h // 2, bytes_accessed=8 * width * two_h, transcendentals=0
        ),
    )(d_in, hidden, w_flat, x_all, dy_all)


def grads_kernel(rep_ref, x_ref, dy_ref, din_ref, hid_ref, gin_ref, gdown_ref, out_ref):
    hidden_units = hid_ref.shape[1]
    xt = x_ref[...].T
    for k in range(2):
        cols = slice(k * hidden_units, (k + 1) * hidden_units)
        own = jnp.dot(xt, din_ref[:, cols], preferred_element_type=jnp.float32)
        out_ref[:, k, :] = (own + gin_ref[:, cols]) * GRAD_SCALE
    own = jnp.dot(dy_ref[...].T, hid_ref[...], preferred_element_type=jnp.float32)
    out_ref[:, 2, :] = (own + gdown_ref[...]) * GRAD_SCALE


def own_grads(rep, x_all, dy_all, d_in, hidden, got_in, got_down, d_tile=256):
    rows, width = x_all.shape
    part, two_h = got_in.shape
    hidden_units = two_h // 2
    n_tiles = part // d_tile
    cols = pl.BlockSpec((rows, d_tile), lambda i, rep: (0, rep[0] * n_tiles + i))
    whole = lambda n: pl.BlockSpec((rows, n), lambda i, rep: (0, 0))
    return pl.pallas_call(
        grads_kernel,
        out_shape=jax.ShapeDtypeStruct((part, 3, hidden_units), jnp.float32),
        grid_spec=pltpu.PrefetchScalarGridSpec(
            num_scalar_prefetch=1,
            grid=(n_tiles,),
            in_specs=[
                cols, cols, whole(two_h), whole(hidden_units),
                pl.BlockSpec((d_tile, two_h), lambda i, rep: (i, 0)),
                pl.BlockSpec((d_tile, hidden_units), lambda i, rep: (i, 0)),
            ],
            out_specs=pl.BlockSpec((d_tile, 3, hidden_units), lambda i, rep: (i, 0, 0)),
        ),
        compiler_params=pltpu.CompilerParams(vmem_limit_bytes=60 * 2**20),
        cost_estimate=pl.CostEstimate(
            flops=6 * rows * part * hidden_units, bytes_accessed=24 * part * hidden_units, transcendentals=0
        ),
    )(rep, x_all, dy_all, d_in, hidden, got_in, got_down)


def cube_code(index, bits):
    if bits < 2:
        return index
    return index ^ ((index >> 1) & (1 << (bits - 2)))


def bit_slice(blocks, axis, value):
    return lax.index_in_dim(blocks, value, axis, keepdims=False)


def copy_block(owners_ref, src_ref, dst_ref):
    dst_ref[...] = src_ref[...]


def reorder(owners, d_in, share):
    n_dp = owners.shape[0]
    width = d_in.shape[1]
    return pl.pallas_call(
        copy_block,
        out_shape=jax.ShapeDtypeStruct(d_in.shape, d_in.dtype),
        grid_spec=pltpu.PrefetchScalarGridSpec(
            num_scalar_prefetch=1,
            grid=(n_dp,),
            in_specs=[pl.BlockSpec((share, width), lambda i, owners: (owners[i], 0))],
            out_specs=pl.BlockSpec((share, width), lambda i, owners: (i, 0)),
        ),
        cost_estimate=pl.CostEstimate(
            flops=0, bytes_accessed=4 * d_in.size, transcendentals=0
        ),
        compiler_params=pltpu.CompilerParams(vmem_limit_bytes=8 * 2**20),
    )(owners, d_in)


def by_permutes(n_dp, n_rep, tokens, cotangent, lengths, w_in, w_down):
    rows = tokens.shape[1]
    width = tokens.shape[2]
    seqs = lengths.shape[1]
    slots = rows // seqs
    hidden_units = w_down.shape[0]
    bits = n_dp.bit_length() - 1
    share = rows // n_dp
    position = jnp.arange(rows)
    owner_seq = (position // slots)[:, None] == jnp.arange(seqs)[None, :]
    limit = jnp.sum(jnp.where(owner_seq, lengths[0][None, :], 0), axis=1)
    is_alive = position % slots < limit
    zero_value = jnp.zeros((), jnp.bfloat16)
    live_x = jnp.where(is_alive[:, None], tokens[0], zero_value)
    live_dy = jnp.where(is_alive[:, None], cotangent[0], zero_value)
    w_flat = lax.optimization_barrier(w_in.reshape(width, 2 * hidden_units))
    gate_up = jnp.dot(live_x, w_flat, preferred_element_type=jnp.float32)
    gate = gate_up[:, :hidden_units]
    upward = gate_up[:, hidden_units:]
    sigmoid_gate = jax.nn.sigmoid(gate)
    activated = gate * sigmoid_gate
    hidden = (activated * upward).astype(jnp.bfloat16)
    d_hidden = lax.dot_general(
        live_dy, w_down, (((1,), (1,)), ((), ())), preferred_element_type=jnp.float32
    )
    d_gate = d_hidden * upward * sigmoid_gate * (1.0 + gate * (1.0 - sigmoid_gate))
    d_up = d_hidden * activated
    d_in = jnp.concatenate([d_gate, d_up], axis=1).astype(jnp.bfloat16)

    me = lax.axis_index("dp")
    my_code = cube_code(me, bits)
    owners = cube_code(my_code ^ jnp.arange(n_dp, dtype=jnp.int32), bits)
    blocks = reorder(owners, d_in, share)
    blocks = blocks.reshape((2,) * bits + (share, 2 * hidden_units))

    n_chunks = bits * COPIES_PER_ORDER
    while width % n_chunks:
        n_chunks -= 1
    columns = width // n_chunks
    flows = []
    for chunk in range(n_chunks):
        order = [(chunk + step) % bits for step in range(bits)]
        weights = lax.slice_in_dim(w_flat, chunk * columns, (chunk + 1) * columns, axis=0)

        def product(part, weights=weights):
            return lax.dot_general(
                part, weights, (((part.ndim - 1,), (1,)), ((), ())), preferred_element_type=jnp.float32
            )

        axis = bits - 1 - order[0]
        sent = product(bit_slice(blocks, axis, 1))
        kept = product(bit_slice(blocks, axis, 0))
        flows.append((order, sent, kept))

    def partner_pairs(bit):
        return [(d, cube_code(cube_code(d, bits) ^ (1 << bit), bits)) for d in range(n_dp)]

    part = width // n_rep
    rep = lax.axis_index("rep")

    def gradients(owner, after):
        x_all, dy_all, d_all, h_all, _ = lax.optimization_barrier((live_x, live_dy, d_in, hidden, after))
        x_part = lax.dynamic_slice_in_dim(x_all, owner * part, part, 1)
        dy_part = lax.dynamic_slice_in_dim(dy_all, owner * part, part, 1)
        pairs = (
            (x_part, d_all[:, :hidden_units]),
            (x_part, d_all[:, hidden_units:]),
            (dy_part, h_all),
        )
        return lax.optimization_barrier(
            tuple(
                lax.dot_general(
                    rows_of, units, (((0,), (0,)), ((), ())), preferred_element_type=jnp.float32
                )
                for rows_of, units in pairs
            )
        )

    first_sent = tuple(sent for _, sent, _ in flows)
    totals = [[], [], []]
    for shift in range(1, n_rep):
        ring = [(r, (r + shift) % n_rep) for r in range(n_rep)]
        for kind, grad in enumerate(gradients((rep + shift) % n_rep, first_sent)):
            totals[kind].append(lax.ppermute(grad, "rep", ring))

    results = [None] * n_chunks
    state = {}
    for chunk, (order, sent, kept) in enumerate(flows):
        state[chunk] = (sent, kept, sorted(order, reverse=True))
    shared = None
    for step in range(bits):
        if step == 1:
            own = gradients(rep, tuple(state[chunk][0] for chunk in range(min(bits, n_chunks))))
            for kind in range(3):
                totals[kind].append(own[kind])
            shared = jnp.stack([sum(terms[1:], terms[0]) for terms in totals], axis=1) * GRAD_SCALE
        for chunk in range(n_chunks):
            order = flows[chunk][0]
            sent, kept, left = state[chunk]
            if step == bits - 1 and shared is not None and chunk >= n_chunks // 2:
                sent, _ = lax.optimization_barrier((sent, shared))
            got = lax.ppermute(sent, "dp", partner_pairs(order[step]))
            left = [b for b in left if b != order[step]]
            if step == bits - 1:
                results[chunk] = kept + got
            else:
                axis = left.index(order[step + 1])
                sent = bit_slice(kept, axis, 1) + bit_slice(got, axis, 1)
                kept = bit_slice(kept, axis, 0) + bit_slice(got, axis, 0)
                state[chunk] = (sent, kept, left)
    shard = jnp.concatenate(results, axis=1)
    return (shard[None], shared)


def by_kernels(n_dp, n_rep, tokens, cotangent, lengths, w_in, w_down):
    rows = tokens.shape[1]
    width = tokens.shape[2]
    seqs = lengths.shape[1]
    slots = rows // seqs
    hidden_units = w_down.shape[0]
    position = jnp.arange(rows)
    owner_seq = (position // slots)[:, None] == jnp.arange(seqs)[None, :]
    limit = jnp.sum(jnp.where(owner_seq, lengths[0][None, :], 0), axis=1)
    is_alive = (position % slots < limit)[:, None]
    w_flat = lax.optimization_barrier(w_in.reshape(width, 2 * hidden_units))
    gate_up = jnp.dot(tokens[0], w_flat, preferred_element_type=jnp.float32)
    gate = gate_up[:, :hidden_units]
    upward = gate_up[:, hidden_units:]
    sigmoid_gate = jax.nn.sigmoid(gate)
    activated = gate * sigmoid_gate
    hidden = jnp.where(is_alive, activated * upward, 0.0).astype(jnp.bfloat16)
    d_hidden = lax.dot_general(
        cotangent[0], w_down, (((1,), (1,)), ((), ())), preferred_element_type=jnp.float32
    )
    d_hidden = jnp.where(is_alive, d_hidden, 0.0)
    d_gate = d_hidden * upward * sigmoid_gate * (1.0 + gate * (1.0 - sigmoid_gate))
    d_up = d_hidden * activated
    d_in = jnp.concatenate([d_gate, d_up], axis=1).astype(jnp.bfloat16)

    shard, got_in, got_down = exchange(d_in, hidden, w_flat, tokens[0], cotangent[0], n_dp, n_rep)
    rep = lax.axis_index("rep").astype(jnp.int32)[None]
    grads = own_grads(rep, tokens[0], cotangent[0], d_in, hidden, got_in, got_down)
    return (shard[None], grads)


def fits_kernels(n_dp, n_rep, rows, width, hidden_units):
    return (
        n_rep == 2
        and n_dp == LINE * NY * NX
        and rows % (8 * n_dp) == 0
        and width % (n_rep * 256) == 0
        and hidden_units % (2 * LANES) in (0, LANES)
    )


def solution(mesh):
    n_dp = mesh.shape["dp"]
    n_rep = mesh.shape["rep"]

    def body(*args):
        tokens, _, _, _, w_down = args
        fast = fits_kernels(n_dp, n_rep, tokens.shape[1], tokens.shape[2], w_down.shape[0])
        return (by_kernels if fast else by_permutes)(n_dp, n_rep, *args)

    in_specs = (
        P("rep", None, None),
        P("rep", None, None),
        P("rep", None),
        P(None, None, "dp"),
        P("dp", None),
    )
    out_specs = (P("rep", "dp", None), P("rep", None, "dp"))
    return jax.shard_map(
        body, mesh=mesh, in_specs=in_specs, out_specs=out_specs, check_vma=False
    )
```

```python
import functools
import jax
import jax.numpy as jnp
from jax import lax
from jax.experimental import pallas as pl
from jax.experimental.pallas import tpu as pltpu

from jax.sharding import PartitionSpec as P

GRAD_SCALE = 0.03125
COPIES_PER_ORDER = 2
MESH = pl.DeviceIdType.MESH
LINE = 4
NY = 2
NX = 2
LANES = 128
PLANE_FIRST_STAGES = (0, 3, 6, 8, 10, 12)
ROW_TILE = 256
UNIT_TILE = 256
LINE_FIRST_GAP = 2
LINE_FIRST_SHARE = 4


def add_blocks(dst, src, lead):
    count = 1
    for n in lead:
        count *= n

    def body(i, carry):
        idx = []
        for n in reversed(lead):
            idx.append(lax.rem(i, n))
            i = i // n
        idx = tuple(reversed(idx))
        dst[idx] = dst[idx] + src[idx]
        return carry

    if count == 1:
        dst[...] = dst[...] + src[...]
    else:
        lax.fori_loop(0, count, body, 0)


def exchange_kernel(
    dims, d_in, hidden, w_ref, x_ref, dy_ref, out_ref, g_in, g_down,
    pa, rs1, rs2, zr, zl, pb, br, bl, bx, by, wbuf, xbuf, tin, tdown,
    s1s, s1r, s2s, s2r, zrs, zrr, zls, zlr, brs, brr, bls, blr, bxs, bxr, bys, byr,
    wsem, xsem, tis, tir, tds, tdr,
):
    nz, n_pairs, n_line, share, d_tile, n_tiles = dims
    d = lax.axis_index("dp")
    rep = lax.axis_index("rep")
    z, y, x = d // (NY * NX), lax.rem(d // NX, NY), lax.rem(d, NX)
    px = d + 1 - 2 * x
    py = d + NX * (1 - 2 * y)
    up, down = d + NY * NX, d - NY * NX
    has_up, has_down = z < nz - 1, z > 0
    other = 1 - rep
    width = 2 * LANES
    rows = d_in.shape[0]
    m_tile = NY * NX * share
    part = n_tiles * d_tile

    barrier = pltpu.get_barrier_semaphore()
    for peer in (px, py):
        pl.semaphore_signal(barrier, inc=1, device_id=(peer, rep), device_id_type=MESH)
    pl.semaphore_signal(barrier, inc=1, device_id=(d, other), device_id_type=MESH)

    @pl.when(has_up)
    def _():
        pl.semaphore_signal(barrier, inc=1, device_id=(up, rep), device_id_type=MESH)

    @pl.when(has_down)
    def _():
        pl.semaphore_signal(barrier, inc=1, device_id=(down, rep), device_id_type=MESH)

    pl.semaphore_wait(barrier, 3 + has_up.astype(jnp.int32) + has_down.astype(jnp.int32))

    def remote(src, dst, ssem, rsem, dev, core=None):
        return pltpu.make_async_remote_copy(
            src_ref=src, dst_ref=dst, send_sem=ssem, recv_sem=rsem,
            device_id=(dev, rep if core is None else core), device_id_type=MESH,
        )

    def first_x(p):
        return remote(pa.at[p, 0, :, :, 1 - x], rs1.at[p, 0], s1s.at[p, 0], s1r.at[p, 0], px)

    def first_y(p):
        return remote(pa.at[p, 1, :, 1 - y], rs1.at[p, 1], s1s.at[p, 1], s1r.at[p, 1], py)

    def second_y(p):
        return remote(pa.at[p, 0, :, 1 - y, x], rs2.at[p, 0], s2s.at[p, 0], s2r.at[p, 0], py)

    def second_x(p):
        return remote(pa.at[p, 1, :, y, 1 - x], rs2.at[p, 1], s2s.at[p, 1], s2r.at[p, 1], px)

    def line_up(p, k):
        return remote(pa.at[p, :, k, y, x], zr.at[p, k], zrs.at[p, k], zrr.at[p, k], up)

    def line_down(p, k):
        return remote(pa.at[p, :, k, y, x], zl.at[p, k], zls.at[p, k], zlr.at[p, k], down)

    def b_up(b, k):
        return remote(pb.at[b, k], br.at[b, k], brs.at[b, k], brr.at[b, k], up)

    def b_down(b, k):
        return remote(pb.at[b, k], bl.at[b, k], bls.at[b, k], blr.at[b, k], down)

    def b_y(b):
        return remote(pb.at[b, z, 1 - y], by.at[b], bys.at[b], byr.at[b], py)

    def b_x(b):
        return remote(pb.at[b, z, y, 1 - x], bx.at[b], bxs.at[b], bxr.at[b], px)

    def w_copy(c):
        slot = lax.rem(c, 2)
        return pltpu.make_async_copy(w_ref.at[pl.ds(c * width, width)], wbuf.at[slot], wsem.at[slot])

    n_chunks = n_pairs + n_line
    w_copy(0).start()

    def product(c, store):
        w_copy(c).wait()

        @pl.when(c + 1 < n_chunks)
        def _():
            w_copy(c + 1).start()

        slot = lax.rem(c, 2)

        def body(k, carry):
            val = lax.dot_general(
                d_in[pl.ds(pl.multiple_of(k * m_tile, m_tile), m_tile), :], wbuf[slot],
                (((1,), (1,)), ((), ())), preferred_element_type=jnp.float32,
            )
            store(k, val)
            return carry

        lax.fori_loop(0, nz, body, 0)

    def store_pair(p):
        def store(k, val):
            val = val.reshape(NY, NX, share, width)
            pa[p, 0, k] = val[..., :LANES]
            pa[p, 1, k] = val[..., LANES:]
        return store

    def store_line(b):
        def store(k, val):
            pb[b, k] = val.reshape(NY, NX, share, width)
        return store

    def x_copy(i, src, s):
        off = pl.multiple_of(other * part + i * d_tile, d_tile)
        return pltpu.make_async_copy(src.at[:, pl.ds(off, d_tile)], xbuf.at[s], xsem.at[s])

    def tin_send(i):
        slot = lax.rem(i, 2)
        return remote(tin.at[slot], g_in.at[pl.ds(i * d_tile, d_tile)], tis.at[slot], tir.at[i], d, other)

    def tdown_send(i):
        slot = lax.rem(i, 2)
        return remote(tdown.at[slot], g_down.at[pl.ds(i * d_tile, d_tile)], tds.at[slot], tdr.at[i], d, other)

    def tile(i):
        x_copy(i, x_ref, 0).wait()
        x_copy(i, dy_ref, 1).wait()
        slot = lax.rem(i, 2)

        @pl.when(i >= 2)
        def _():
            tin_send(i - 2).wait_send()
            tdown_send(i - 2).wait_send()

        n_w = LANES
        lhs = xbuf[0].T

        def body(n, carry):
            cols = pl.ds(pl.multiple_of(n * width, width), width)
            tin[slot, :, cols] = jnp.dot(lhs, d_in[:, cols], preferred_element_type=jnp.float32)
            return carry

        lax.fori_loop(0, d_in.shape[1] // width, body, 0)
        lhs2 = xbuf[1].T
        tdown[slot] = jnp.dot(lhs2, hidden[...], preferred_element_type=jnp.float32)

        @pl.when(i + 1 < n_tiles)
        def _():
            x_copy(i + 1, x_ref, 0).start()
            x_copy(i + 1, dy_ref, 1).start()

        tin_send(i).start()
        tdown_send(i).start()

    x_copy(0, x_ref, 0).start()
    x_copy(0, dy_ref, 1).start()

    def a0(p):
        product(p + jnp.minimum(lax.div(p, LINE_FIRST_GAP) + 1, n_line), store_pair(p))
        first_x(p).start()
        first_y(p).start()

    def a1(p):
        first_x(p).wait_recv()
        add_blocks(pa.at[p, 0, :, 1 - y, x], rs1.at[p, 0, :, 1 - y], (nz,))
        second_y(p).start()
        first_y(p).wait_recv()
        add_blocks(pa.at[p, 1, :, y, 1 - x], rs1.at[p, 1, :, 1 - x], (nz,))
        second_x(p).start()
        add_blocks(pa.at[p, 0, :, y, x], rs1.at[p, 0, :, y], (nz,))
        add_blocks(pa.at[p, 1, :, y, x], rs1.at[p, 1, :, x], (nz,))

    def a2(p):
        second_y(p).wait_recv()
        add_blocks(pa.at[p, 0, :, y, x], rs2.at[p, 0], (nz,))
        second_x(p).wait_recv()
        add_blocks(pa.at[p, 1, :, y, x], rs2.at[p, 1], (nz,))
        hop_send(0, functools.partial(line_up, p), functools.partial(line_down, p), None, None)

    def hop_send(h, cup, cdown, add_up, add_down):
        @pl.when(z == h)
        def _():
            for k in range(nz - 1, h, -1):
                if h:
                    cup(k).wait_recv()
                    add_up(k)
                cup(k).start()

        @pl.when(z == nz - 1 - h)
        def _():
            for k in range(0, nz - 1 - h):
                if h:
                    cdown(k).wait_recv()
                    add_down(k)
                cdown(k).start()

    def a_hop(h):
        def go(p):
            hop_send(
                h, functools.partial(line_up, p), functools.partial(line_down, p),
                lambda k: add_blocks(pa.at[p, :, k, y, x], zr.at[p, k], (2,)),
                lambda k: add_blocks(pa.at[p, :, k, y, x], zl.at[p, k], (2,)),
            )
        return go

    def a_last(p):
        @pl.when(has_down)
        def _():
            line_up(p, z).wait_recv()
            add_blocks(pa.at[p, :, z, y, x], zr.at[p, z], (2,))

        @pl.when(has_up)
        def _():
            line_down(p, z).wait_recv()
            add_blocks(pa.at[p, :, z, y, x], zl.at[p, z], (2,))

        c = p + jnp.minimum(lax.div(p, LINE_FIRST_GAP) + 1, n_line)
        for u in range(2):
            cols = pl.ds(pl.multiple_of(c * width + u * LANES, LANES), LANES)
            out_ref[:, cols] = pa[p, u, z, y, x]

    def b_chunk(b):
        return b * (LINE_FIRST_GAP + 1)

    def b0(b):
        product(b_chunk(b), store_line(b))
        hop_send(0, functools.partial(b_up, b), functools.partial(b_down, b), None, None)

    def b_hop(h):
        def go(b):
            hop_send(
                h, functools.partial(b_up, b), functools.partial(b_down, b),
                lambda k: add_blocks(pb.at[b, k], br.at[b, k], (NY, NX)),
                lambda k: add_blocks(pb.at[b, k], bl.at[b, k], (NY, NX)),
            )
        return go

    def b_plane(b):
        @pl.when(has_down)
        def _():
            b_up(b, z).wait_recv()
            add_blocks(pb.at[b, z], br.at[b, z], (NY, NX))

        @pl.when(has_up)
        def _():
            b_down(b, z).wait_recv()
            add_blocks(pb.at[b, z], bl.at[b, z], (NY, NX))

        b_y(b).start()

    def b_second(b):
        b_y(b).wait_recv()
        add_blocks(pb.at[b, z, y], by.at[b], (NX,))
        b_x(b).start()

    def b_last(b):
        b_x(b).wait_recv()
        cols = pl.ds(pl.multiple_of(b_chunk(b) * width, width), width)
        out_ref[:, cols] = pb[b, z, y, x] + bx[b]

    hops = nz - 1
    a_stages = [a0, a1, a2] + [a_hop(h) for h in range(1, hops)] + [a_last]
    b_stages = [b0] + [b_hop(h) for h in range(1, hops)] + [b_plane, b_second, b_last]
    a_at = PLANE_FIRST_STAGES
    b_at = [2 * j for j in range(len(b_stages))]
    n_steps = max(n_pairs + a_at[-1], (n_line - 1) * LINE_FIRST_GAP + b_at[-1] + 1, n_tiles)

    def step(t, carry):
        def run_b(j):
            s = t - b_at[j]

            @pl.when((s >= 0) & (lax.rem(s, LINE_FIRST_GAP) == 0) & (lax.div(s, LINE_FIRST_GAP) < n_line))
            def _():
                b_stages[j](lax.div(s, LINE_FIRST_GAP))

        def run_a(j):
            s = t - a_at[j]

            @pl.when((s >= 0) & (s < n_pairs))
            def _():
                a_stages[j](s)

        run_b(0)
        run_a(0)

        @pl.when(t < n_tiles)
        def _():
            tile(t)

        for j in range(1, len(a_stages)):
            run_a(j)
        for j in range(1, len(b_stages)):
            run_b(j)
        return carry

    lax.fori_loop(0, n_steps, step, 0)

    def drain(p, carry):
        for c in (first_x, first_y, second_y, second_x):
            c(p).wait_send()
        for k in range(nz):
            @pl.when(k > z)
            def _():
                line_up(p, k).wait_send()

            @pl.when(k < z)
            def _():
                line_down(p, k).wait_send()
        return carry

    lax.fori_loop(0, n_pairs, drain, 0)

    def drain_b(b, carry):
        b_y(b).wait_send()
        b_x(b).wait_send()
        for k in range(nz):
            @pl.when(k > z)
            def _():
                b_up(b, k).wait_send()

            @pl.when(k < z)
            def _():
                b_down(b, k).wait_send()
        return carry

    lax.fori_loop(0, n_line, drain_b, 0)
    for i in range(max(n_tiles - 2, 0), n_tiles):
        tin_send(i).wait_send()
        tdown_send(i).wait_send()

    def drain_t(i, carry):
        tin_send(i).wait_recv()
        tdown_send(i).wait_recv()
        return carry

    lax.fori_loop(0, n_tiles, drain_t, 0)


def exchange(d_in, hidden, w_flat, x_all, dy_all, n_dp, n_rep):
    rows, two_h = d_in.shape
    width = w_flat.shape[0]
    nz = n_dp // (NY * NX)
    share = rows // n_dp
    n_chunks = width // (2 * LANES)
    n_line = n_chunks // LINE_FIRST_SHARE
    n_pairs = n_chunks - n_line
    part = width // n_rep
    d_tile = 256
    n_tiles = part // d_tile
    dims = (nz, n_pairs, n_line, share, d_tile, n_tiles)
    f32 = jnp.float32
    dma = pltpu.SemaphoreType.DMA
    wide = 2 * LANES
    return pl.pallas_call(
        functools.partial(exchange_kernel, dims),
        out_shape=(
            jax.ShapeDtypeStruct((share, width), f32),
            jax.ShapeDtypeStruct((part, two_h), f32),
            jax.ShapeDtypeStruct((part, two_h // 2), f32),
        ),
        in_specs=[pl.BlockSpec(memory_space=pltpu.VMEM)] * 2 + [pl.BlockSpec(memory_space=pl.ANY)] * 3,
        out_specs=(
            pl.BlockSpec(memory_space=pltpu.VMEM),
            pl.BlockSpec(memory_space=pl.ANY),
            pl.BlockSpec(memory_space=pl.ANY),
        ),
        scratch_shapes=[
            pltpu.VMEM((n_pairs, 2, nz, NY, NX, share, LANES), f32),
            pltpu.VMEM((n_pairs, 2, nz, 2, share, LANES), f32),
            pltpu.VMEM((n_pairs, 2, nz, share, LANES), f32),
            pltpu.VMEM((n_pairs, nz, 2, share, LANES), f32),
            pltpu.VMEM((n_pairs, nz, 2, share, LANES), f32),
            pltpu.VMEM((n_line, nz, NY, NX, share, wide), f32),
            pltpu.VMEM((n_line, nz, NY, NX, share, wide), f32),
            pltpu.VMEM((n_line, nz, NY, NX, share, wide), f32),
            pltpu.VMEM((n_line, share, wide), f32),
            pltpu.VMEM((n_line, NX, share, wide), f32),
            pltpu.VMEM((2, wide, two_h), jnp.bfloat16),
            pltpu.VMEM((2, rows, d_tile), jnp.bfloat16),
            pltpu.VMEM((2, d_tile, two_h), f32),
            pltpu.VMEM((2, d_tile, two_h // 2), f32),
            dma((n_pairs, 2)), dma((n_pairs, 2)), dma((n_pairs, 2)), dma((n_pairs, 2)),
            dma((n_pairs, nz)), dma((n_pairs, nz)), dma((n_pairs, nz)), dma((n_pairs, nz)),
            dma((n_line, nz)), dma((n_line, nz)), dma((n_line, nz)), dma((n_line, nz)),
            dma((n_line,)), dma((n_line,)), dma((n_line,)), dma((n_line,)),
            dma((2,)), dma((2,)), dma((2,)), dma((n_tiles,)), dma((2,)), dma((n_tiles,)),
        ],
        compiler_params=pltpu.CompilerParams(
            collective_id=0, has_side_effects=True, vmem_limit_bytes=62 * 2**20
        ),
        cost_estimate=pl.CostEstimate(
            flops=5 * rows * width * two_h // 2, bytes_accessed=8 * width * two_h, transcendentals=0
        ),
    )(d_in, hidden, w_flat, x_all, dy_all)


def unit_tiles(hidden_units):
    starts = range(0, hidden_units, UNIT_TILE)
    return [(u, min(UNIT_TILE, hidden_units - u)) for u in starts]


def units_kernel(tiles_per_seq, lens_ref, x_ref, dy_ref, w_ref, wd_ref, din_ref, hid_ref, wv, wdv, sems):
    m = pl.program_id(0)
    hidden_units = wd_ref.shape[0]
    pieces = unit_tiles(hidden_units)

    def copies(j):
        u, n = pieces[j]
        return (
            pltpu.make_async_copy(w_ref.at[:, pl.ds(u, n)], wv.at[:, pl.ds(u, n)], sems.at[3 * j]),
            pltpu.make_async_copy(
                w_ref.at[:, pl.ds(hidden_units + u, n)], wv.at[:, pl.ds(hidden_units + u, n)], sems.at[3 * j + 1]
            ),
            pltpu.make_async_copy(wd_ref.at[pl.ds(u, n)], wdv.at[pl.ds(u, n)], sems.at[3 * j + 2]),
        )

    @pl.when(m == 0)
    def _():
        for j in range(len(pieces)):
            for c in copies(j):
                c.start()

    seq = m // tiles_per_seq
    live = lens_ref[seq] - lax.rem(m, tiles_per_seq) * x_ref.shape[0]

    for j, (u, n) in enumerate(pieces):
        @pl.when(m == 0)
        def _():
            for c in copies(j):
                c.wait()

        lo = slice(u, u + n)
        hi = slice(hidden_units + u, hidden_units + u + n)

        @pl.when(live > 0)
        def _():
            gate = jnp.dot(x_ref[...], wv[:, lo], preferred_element_type=jnp.float32)
            upward = jnp.dot(x_ref[...], wv[:, hi], preferred_element_type=jnp.float32)
            d_hidden = lax.dot_general(
                dy_ref[...], wdv[lo, :], (((1,), (1,)), ((), ())), preferred_element_type=jnp.float32
            )
            alive = lax.broadcasted_iota(jnp.int32, gate.shape, 0) < live
            d_hidden = jnp.where(alive, d_hidden, 0.0)
            sigmoid_gate = jax.nn.sigmoid(gate)
            activated = gate * sigmoid_gate
            hid_ref[:, lo] = jnp.where(alive, activated * upward, 0.0).astype(jnp.bfloat16)
            d_gate = d_hidden * upward * sigmoid_gate * (1.0 + gate * (1.0 - sigmoid_gate))
            din_ref[:, lo] = d_gate.astype(jnp.bfloat16)
            din_ref[:, hi] = (d_hidden * activated).astype(jnp.bfloat16)

    @pl.when(live <= 0)
    def _():
        hid_ref[...] = jnp.zeros_like(hid_ref)
        din_ref[...] = jnp.zeros_like(din_ref)


def unit_grads(lens, x_all, dy_all, w_flat, w_down):
    rows, width = x_all.shape
    hidden_units = w_down.shape[0]
    tiles_per_seq = rows // lens.shape[0] // ROW_TILE
    n_sems = 3 * len(unit_tiles(hidden_units))
    row_block = lambda n: pl.BlockSpec((ROW_TILE, n), lambda m, lens: (m, 0))
    return pl.pallas_call(
        functools.partial(units_kernel, tiles_per_seq),
        out_shape=(
            jax.ShapeDtypeStruct((rows, 2 * hidden_units), jnp.bfloat16),
            jax.ShapeDtypeStruct((rows, hidden_units), jnp.bfloat16),
        ),
        grid_spec=pltpu.PrefetchScalarGridSpec(
            num_scalar_prefetch=1,
            grid=(rows // ROW_TILE,),
            in_specs=[row_block(width), row_block(width)] + [pl.BlockSpec(memory_space=pl.ANY)] * 2,
            out_specs=(row_block(2 * hidden_units), row_block(hidden_units)),
            scratch_shapes=[
                pltpu.VMEM((width, 2 * hidden_units), jnp.bfloat16),
                pltpu.VMEM((hidden_units, width), jnp.bfloat16),
                pltpu.SemaphoreType.DMA((n_sems,)),
            ],
        ),
        compiler_params=pltpu.CompilerParams(vmem_limit_bytes=60 * 2**20),
        cost_estimate=pl.CostEstimate(
            flops=6 * rows * width * hidden_units, bytes_accessed=6 * width * hidden_units, transcendentals=0
        ),
    )(lens, x_all, dy_all, w_flat, w_down)


def grads_kernel(rep_ref, x_ref, dy_ref, din_ref, hid_ref, gin_ref, gdown_ref, out_ref):
    hidden_units = hid_ref.shape[1]
    xt = x_ref[...].T
    for k in range(2):
        cols = slice(k * hidden_units, (k + 1) * hidden_units)
        own = jnp.dot(xt, din_ref[:, cols], preferred_element_type=jnp.float32)
        out_ref[k] = (own + gin_ref[:, cols]) * GRAD_SCALE
    own = jnp.dot(dy_ref[...].T, hid_ref[...], preferred_element_type=jnp.float32)
    out_ref[2] = (own + gdown_ref[...]) * GRAD_SCALE


def own_grads(rep, x_all, dy_all, d_in, hidden, got_in, got_down, d_tile=256):
    rows, width = x_all.shape
    part, two_h = got_in.shape
    hidden_units = two_h // 2
    n_tiles = part // d_tile
    cols = pl.BlockSpec((rows, d_tile), lambda i, rep: (0, rep[0] * n_tiles + i))
    whole = lambda n: pl.BlockSpec((rows, n), lambda i, rep: (0, 0))
    return pl.pallas_call(
        grads_kernel,
        out_shape=jax.ShapeDtypeStruct((3, part, hidden_units), jnp.float32),
        grid_spec=pltpu.PrefetchScalarGridSpec(
            num_scalar_prefetch=1,
            grid=(n_tiles,),
            in_specs=[
                cols, cols, whole(two_h), whole(hidden_units),
                pl.BlockSpec((d_tile, two_h), lambda i, rep: (i, 0)),
                pl.BlockSpec((d_tile, hidden_units), lambda i, rep: (i, 0)),
            ],
            out_specs=pl.BlockSpec((3, d_tile, hidden_units), lambda i, rep: (0, i, 0)),
        ),
        compiler_params=pltpu.CompilerParams(vmem_limit_bytes=60 * 2**20),
        cost_estimate=pl.CostEstimate(
            flops=6 * rows * part * hidden_units, bytes_accessed=24 * part * hidden_units, transcendentals=0
        ),
    )(rep, x_all, dy_all, d_in, hidden, got_in, got_down)


def cube_code(index, bits):
    if bits < 2:
        return index
    return index ^ ((index >> 1) & (1 << (bits - 2)))


def bit_slice(blocks, axis, value):
    return lax.index_in_dim(blocks, value, axis, keepdims=False)


def copy_block(owners_ref, src_ref, dst_ref):
    dst_ref[...] = src_ref[...]


def reorder(owners, d_in, share):
    n_dp = owners.shape[0]
    width = d_in.shape[1]
    return pl.pallas_call(
        copy_block,
        out_shape=jax.ShapeDtypeStruct(d_in.shape, d_in.dtype),
        grid_spec=pltpu.PrefetchScalarGridSpec(
            num_scalar_prefetch=1,
            grid=(n_dp,),
            in_specs=[pl.BlockSpec((share, width), lambda i, owners: (owners[i], 0))],
            out_specs=pl.BlockSpec((share, width), lambda i, owners: (i, 0)),
        ),
        cost_estimate=pl.CostEstimate(
            flops=0, bytes_accessed=4 * d_in.size, transcendentals=0
        ),
        compiler_params=pltpu.CompilerParams(vmem_limit_bytes=8 * 2**20),
    )(owners, d_in)


def by_permutes(n_dp, n_rep, tokens, cotangent, lengths, w_in, w_down):
    rows = tokens.shape[1]
    width = tokens.shape[2]
    seqs = lengths.shape[1]
    slots = rows // seqs
    hidden_units = w_down.shape[0]
    bits = n_dp.bit_length() - 1
    share = rows // n_dp
    position = jnp.arange(rows)
    owner_seq = (position // slots)[:, None] == jnp.arange(seqs)[None, :]
    limit = jnp.sum(jnp.where(owner_seq, lengths[0][None, :], 0), axis=1)
    is_alive = position % slots < limit
    zero_value = jnp.zeros((), jnp.bfloat16)
    live_x = jnp.where(is_alive[:, None], tokens[0], zero_value)
    live_dy = jnp.where(is_alive[:, None], cotangent[0], zero_value)
    w_flat = lax.optimization_barrier(w_in.reshape(width, 2 * hidden_units))
    gate_up = jnp.dot(live_x, w_flat, preferred_element_type=jnp.float32)
    gate = gate_up[:, :hidden_units]
    upward = gate_up[:, hidden_units:]
    sigmoid_gate = jax.nn.sigmoid(gate)
    activated = gate * sigmoid_gate
    hidden = (activated * upward).astype(jnp.bfloat16)
    d_hidden = lax.dot_general(
        live_dy, w_down, (((1,), (1,)), ((), ())), preferred_element_type=jnp.float32
    )
    d_gate = d_hidden * upward * sigmoid_gate * (1.0 + gate * (1.0 - sigmoid_gate))
    d_up = d_hidden * activated
    d_in = jnp.concatenate([d_gate, d_up], axis=1).astype(jnp.bfloat16)

    me = lax.axis_index("dp")
    my_code = cube_code(me, bits)
    owners = cube_code(my_code ^ jnp.arange(n_dp, dtype=jnp.int32), bits)
    blocks = reorder(owners, d_in, share)
    blocks = blocks.reshape((2,) * bits + (share, 2 * hidden_units))

    n_chunks = bits * COPIES_PER_ORDER
    while width % n_chunks:
        n_chunks -= 1
    columns = width // n_chunks
    flows = []
    for chunk in range(n_chunks):
        order = [(chunk + step) % bits for step in range(bits)]
        weights = lax.slice_in_dim(w_flat, chunk * columns, (chunk + 1) * columns, axis=0)

        def product(part, weights=weights):
            return lax.dot_general(
                part, weights, (((part.ndim - 1,), (1,)), ((), ())), preferred_element_type=jnp.float32
            )

        axis = bits - 1 - order[0]
        sent = product(bit_slice(blocks, axis, 1))
        kept = product(bit_slice(blocks, axis, 0))
        flows.append((order, sent, kept))

    def partner_pairs(bit):
        return [(d, cube_code(cube_code(d, bits) ^ (1 << bit), bits)) for d in range(n_dp)]

    part = width // n_rep
    rep = lax.axis_index("rep")

    def gradients(owner, after):
        x_all, dy_all, d_all, h_all, _ = lax.optimization_barrier((live_x, live_dy, d_in, hidden, after))
        x_part = lax.dynamic_slice_in_dim(x_all, owner * part, part, 1)
        dy_part = lax.dynamic_slice_in_dim(dy_all, owner * part, part, 1)
        pairs = (
            (x_part, d_all[:, :hidden_units]),
            (x_part, d_all[:, hidden_units:]),
            (dy_part, h_all),
        )
        return lax.optimization_barrier(
            tuple(
                lax.dot_general(
                    rows_of, units, (((0,), (0,)), ((), ())), preferred_element_type=jnp.float32
                )
                for rows_of, units in pairs
            )
        )

    first_sent = tuple(sent for _, sent, _ in flows)
    totals = [[], [], []]
    for shift in range(1, n_rep):
        ring = [(r, (r + shift) % n_rep) for r in range(n_rep)]
        for kind, grad in enumerate(gradients((rep + shift) % n_rep, first_sent)):
            totals[kind].append(lax.ppermute(grad, "rep", ring))

    results = [None] * n_chunks
    state = {}
    for chunk, (order, sent, kept) in enumerate(flows):
        state[chunk] = (sent, kept, sorted(order, reverse=True))
    shared = None
    for step in range(bits):
        if step == 1:
            own = gradients(rep, tuple(state[chunk][0] for chunk in range(min(bits, n_chunks))))
            for kind in range(3):
                totals[kind].append(own[kind])
            shared = jnp.stack([sum(terms[1:], terms[0]) for terms in totals], axis=1) * GRAD_SCALE
        for chunk in range(n_chunks):
            order = flows[chunk][0]
            sent, kept, left = state[chunk]
            if step == bits - 1 and shared is not None and chunk >= n_chunks // 2:
                sent, _ = lax.optimization_barrier((sent, shared))
            got = lax.ppermute(sent, "dp", partner_pairs(order[step]))
            left = [b for b in left if b != order[step]]
            if step == bits - 1:
                results[chunk] = kept + got
            else:
                axis = left.index(order[step + 1])
                sent = bit_slice(kept, axis, 1) + bit_slice(got, axis, 1)
                kept = bit_slice(kept, axis, 0) + bit_slice(got, axis, 0)
                state[chunk] = (sent, kept, left)
    shard = jnp.concatenate(results, axis=1)
    return (shard[None], shared)


def by_kernels(n_dp, n_rep, tokens, cotangent, lengths, w_in, w_down):
    width = tokens.shape[2]
    hidden_units = w_down.shape[0]
    w_flat = lax.optimization_barrier(w_in.reshape(width, 2 * hidden_units))
    d_in, hidden = unit_grads(lengths[0], tokens[0], cotangent[0], w_flat, w_down)
    shard, got_in, got_down = exchange(d_in, hidden, w_flat, tokens[0], cotangent[0], n_dp, n_rep)
    rep = lax.axis_index("rep").astype(jnp.int32)[None]
    grads = own_grads(rep, tokens[0], cotangent[0], d_in, hidden, got_in, got_down)
    return (shard[None], grads.transpose(1, 0, 2))


def fits_kernels(n_dp, n_rep, rows, seqs, width, hidden_units):
    return (
        n_rep == 2
        and n_dp == LINE * NY * NX
        and rows % (16 * n_dp) == 0
        and rows % (seqs * ROW_TILE) == 0
        and width % (n_rep * 256) == 0
        and hidden_units % (2 * LANES) in (0, LANES)
    )


def solution(mesh):
    n_dp = mesh.shape["dp"]
    n_rep = mesh.shape["rep"]

    def body(*args):
        tokens, _, _, _, w_down = args
        fast = fits_kernels(n_dp, n_rep, tokens.shape[1], args[2].shape[1], tokens.shape[2], w_down.shape[0])
        return (by_kernels if fast else by_permutes)(n_dp, n_rep, *args)

    in_specs = (
        P("rep", None, None),
        P("rep", None, None),
        P("rep", None),
        P(None, None, "dp"),
        P("dp", None),
    )
    out_specs = (P("rep", "dp", None), P("rep", None, "dp"))
    return jax.shard_map(
        body, mesh=mesh, in_specs=in_specs, out_specs=out_specs, check_vma=False
    )
```

```python
import functools
import jax
import jax.numpy as jnp
from jax import lax
from jax.experimental import pallas as pl
from jax.experimental.pallas import tpu as pltpu

from jax.sharding import PartitionSpec as P

GRAD_SCALE = 0.03125
COPIES_PER_ORDER = 2
MESH = pl.DeviceIdType.MESH
LINE = 4
NY = 2
NX = 2
LANES = 128
PLANE_FIRST_STAGES = (0, 3, 6, 9, 11, 13)
LINE_FIRST_STAGES = (0, 4, 7, 13, 15, 17)
ROW_TILE = 256
UNIT_TILE = 256
LINE_FIRST_GAP = 2
LINE_FIRST_SHARE = 4


def add_blocks(dst, src, lead):
    count = 1
    for n in lead:
        count *= n

    def body(i, carry):
        idx = []
        for n in reversed(lead):
            idx.append(lax.rem(i, n))
            i = i // n
        idx = tuple(reversed(idx))
        dst[idx] = dst[idx] + src[idx]
        return carry

    if count == 1:
        dst[...] = dst[...] + src[...]
    else:
        lax.fori_loop(0, count, body, 0)


def exchange_kernel(
    dims, d_in, hidden, w_ref, x_ref, dy_ref, out_ref, total, g_in, g_down,
    pa, rs1, rs2, zr, zl, pb, br, bl, bx, by, wbuf, xbuf, tin, tdown, gin, gdown,
    s1s, s1r, s2s, s2r, zrs, zrr, zls, zlr, brs, brr, bls, blr, bxs, bxr, bys, byr,
    wsem, xsem, tis, tir, tds, tdr, gsem, osem,
):
    nz, n_pairs, n_line, share, d_tile, n_tiles = dims
    d = lax.axis_index("dp")
    rep = lax.axis_index("rep")
    z, y, x = d // (NY * NX), lax.rem(d // NX, NY), lax.rem(d, NX)
    px = d + 1 - 2 * x
    py = d + NX * (1 - 2 * y)
    up, down = d + NY * NX, d - NY * NX
    has_up, has_down = z < nz - 1, z > 0
    other = 1 - rep
    width = 2 * LANES
    rows = d_in.shape[0]
    m_tile = NY * NX * share
    part = n_tiles * d_tile

    barrier = pltpu.get_barrier_semaphore()
    for peer in (px, py):
        pl.semaphore_signal(barrier, inc=1, device_id=(peer, rep), device_id_type=MESH)
    pl.semaphore_signal(barrier, inc=1, device_id=(d, other), device_id_type=MESH)

    @pl.when(has_up)
    def _():
        pl.semaphore_signal(barrier, inc=1, device_id=(up, rep), device_id_type=MESH)

    @pl.when(has_down)
    def _():
        pl.semaphore_signal(barrier, inc=1, device_id=(down, rep), device_id_type=MESH)

    pl.semaphore_wait(barrier, 3 + has_up.astype(jnp.int32) + has_down.astype(jnp.int32))

    def remote(src, dst, ssem, rsem, dev, core=None):
        return pltpu.make_async_remote_copy(
            src_ref=src, dst_ref=dst, send_sem=ssem, recv_sem=rsem,
            device_id=(dev, rep if core is None else core), device_id_type=MESH,
        )

    def first_x(p):
        return remote(pa.at[p, 0, :, :, 1 - x], rs1.at[p, 0], s1s.at[p, 0], s1r.at[p, 0], px)

    def first_y(p):
        return remote(pa.at[p, 1, :, 1 - y], rs1.at[p, 1], s1s.at[p, 1], s1r.at[p, 1], py)

    def second_y(p):
        return remote(pa.at[p, 0, :, 1 - y, x], rs2.at[p, 0], s2s.at[p, 0], s2r.at[p, 0], py)

    def second_x(p):
        return remote(pa.at[p, 1, :, y, 1 - x], rs2.at[p, 1], s2s.at[p, 1], s2r.at[p, 1], px)

    def line_up(p, k):
        return remote(pa.at[p, :, k, y, x], zr.at[p, k], zrs.at[p, k], zrr.at[p, k], up)

    def line_down(p, k):
        return remote(pa.at[p, :, k, y, x], zl.at[p, k], zls.at[p, k], zlr.at[p, k], down)

    def b_up(b, k):
        return remote(pb.at[b, k], br.at[b, k], brs.at[b, k], brr.at[b, k], up)

    def b_down(b, k):
        return remote(pb.at[b, k], bl.at[b, k], bls.at[b, k], blr.at[b, k], down)

    def b_y(b):
        return remote(pb.at[b, z, 1 - y], by.at[b], bys.at[b], byr.at[b], py)

    def b_x(b):
        return remote(pb.at[b, z, y, 1 - x], bx.at[b], bxs.at[b], bxr.at[b], px)

    def w_copy(c):
        slot = lax.rem(c, 2)
        return pltpu.make_async_copy(w_ref.at[pl.ds(c * width, width)], wbuf.at[slot], wsem.at[slot])

    n_chunks = n_pairs + n_line
    w_copy(0).start()

    def product(c, store):
        w_copy(c).wait()

        @pl.when(c + 1 < n_chunks)
        def _():
            w_copy(c + 1).start()

        slot = lax.rem(c, 2)

        def body(k, carry):
            val = lax.dot_general(
                d_in[pl.ds(pl.multiple_of(k * m_tile, m_tile), m_tile), :], wbuf[slot],
                (((1,), (1,)), ((), ())), preferred_element_type=jnp.float32,
            )
            store(k, val)
            return carry

        lax.fori_loop(0, nz, body, 0)

    def store_pair(p):
        def store(k, val):
            val = val.reshape(NY, NX, share, width)
            pa[p, 0, k] = val[..., :LANES]
            pa[p, 1, k] = val[..., LANES:]
        return store

    def store_line(b):
        def store(k, val):
            pb[b, k] = val.reshape(NY, NX, share, width)
        return store

    def x_copy(i, src, s):
        core = jnp.where(i < n_tiles, other, rep)
        off = pl.multiple_of(core * part + lax.rem(i, n_tiles) * d_tile, d_tile)
        return pltpu.make_async_copy(src.at[:, pl.ds(off, d_tile)], xbuf.at[s], xsem.at[s])

    def tin_send(i):
        slot = lax.rem(i, 2)
        return remote(tin.at[slot], g_in.at[pl.ds(i * d_tile, d_tile)], tis.at[slot], tir.at[i], d, other)

    def tdown_send(i):
        slot = lax.rem(i, 2)
        return remote(tdown.at[slot], g_down.at[pl.ds(i * d_tile, d_tile)], tds.at[slot], tdr.at[i], d, other)

    def got_copies(i):
        at = pl.ds(i * d_tile, d_tile)
        return (
            pltpu.make_async_copy(g_in.at[at], gin, gsem.at[0]),
            pltpu.make_async_copy(g_down.at[at], gdown, gsem.at[1]),
        )

    def total_copies(i):
        at = pl.ds(i * d_tile, d_tile)
        units = gdown.shape[1]
        return (
            pltpu.make_async_copy(gin.at[:, pl.ds(0, units)], total.at[0, at], osem.at[0]),
            pltpu.make_async_copy(gin.at[:, pl.ds(units, units)], total.at[1, at], osem.at[1]),
            pltpu.make_async_copy(gdown, total.at[2, at], osem.at[2]),
        )

    def columns(store):
        lhs = xbuf[0].T

        def body(n, carry):
            cols = pl.ds(pl.multiple_of(n * width, width), width)
            store(cols, jnp.dot(lhs, d_in[:, cols], preferred_element_type=jnp.float32))
            return carry

        lax.fori_loop(0, d_in.shape[1] // width, body, 0)
        return jnp.dot(xbuf[1].T, hidden[...], preferred_element_type=jnp.float32)

    def tile(i):
        x_copy(i, x_ref, 0).wait()
        x_copy(i, dy_ref, 1).wait()

        @pl.when(i < n_tiles)
        def _():
            slot = lax.rem(i, 2)

            @pl.when(i >= 2)
            def _():
                tin_send(i - 2).wait_send()
                tdown_send(i - 2).wait_send()

            def store(cols, val):
                tin[slot, :, cols] = val

            tdown[slot] = columns(store)
            tin_send(i).start()
            tdown_send(i).start()

        @pl.when(i >= n_tiles)
        def _():
            k = i - n_tiles

            @pl.when(k >= 1)
            def _():
                for c in total_copies(k - 1):
                    c.wait()

            tin_send(k).wait_recv()
            tdown_send(k).wait_recv()
            for c in got_copies(k):
                c.start()
            for c in got_copies(k):
                c.wait()

            def store(cols, val):
                gin[:, cols] = (gin[:, cols] + val) * GRAD_SCALE

            gdown[...] = (gdown[...] + columns(store)) * GRAD_SCALE
            for c in total_copies(k):
                c.start()

        @pl.when(i + 1 < 2 * n_tiles)
        def _():
            x_copy(i + 1, x_ref, 0).start()
            x_copy(i + 1, dy_ref, 1).start()

    x_copy(0, x_ref, 0).start()
    x_copy(0, dy_ref, 1).start()

    def a0(p):
        product(p + jnp.minimum(lax.div(p, LINE_FIRST_GAP) + 1, n_line), store_pair(p))
        first_x(p).start()
        first_y(p).start()

    def a1(p):
        first_x(p).wait_recv()
        add_blocks(pa.at[p, 0, :, 1 - y, x], rs1.at[p, 0, :, 1 - y], (nz,))
        second_y(p).start()
        first_y(p).wait_recv()
        add_blocks(pa.at[p, 1, :, y, 1 - x], rs1.at[p, 1, :, 1 - x], (nz,))
        second_x(p).start()
        add_blocks(pa.at[p, 0, :, y, x], rs1.at[p, 0, :, y], (nz,))
        add_blocks(pa.at[p, 1, :, y, x], rs1.at[p, 1, :, x], (nz,))

    def a2(p):
        second_y(p).wait_recv()
        add_blocks(pa.at[p, 0, :, y, x], rs2.at[p, 0], (nz,))
        second_x(p).wait_recv()
        add_blocks(pa.at[p, 1, :, y, x], rs2.at[p, 1], (nz,))
        hop_send(0, functools.partial(line_up, p), functools.partial(line_down, p), None, None)

    def hop_send(h, cup, cdown, add_up, add_down):
        @pl.when(z == h)
        def _():
            for k in range(nz - 1, h, -1):
                if h:
                    cup(k).wait_recv()
                    add_up(k)
                cup(k).start()

        @pl.when(z == nz - 1 - h)
        def _():
            for k in range(0, nz - 1 - h):
                if h:
                    cdown(k).wait_recv()
                    add_down(k)
                cdown(k).start()

    def a_hop(h):
        def go(p):
            hop_send(
                h, functools.partial(line_up, p), functools.partial(line_down, p),
                lambda k: add_blocks(pa.at[p, :, k, y, x], zr.at[p, k], (2,)),
                lambda k: add_blocks(pa.at[p, :, k, y, x], zl.at[p, k], (2,)),
            )
        return go

    def a_last(p):
        @pl.when(has_down)
        def _():
            line_up(p, z).wait_recv()
            add_blocks(pa.at[p, :, z, y, x], zr.at[p, z], (2,))

        @pl.when(has_up)
        def _():
            line_down(p, z).wait_recv()
            add_blocks(pa.at[p, :, z, y, x], zl.at[p, z], (2,))

        c = p + jnp.minimum(lax.div(p, LINE_FIRST_GAP) + 1, n_line)
        for u in range(2):
            cols = pl.ds(pl.multiple_of(c * width + u * LANES, LANES), LANES)
            out_ref[:, cols] = pa[p, u, z, y, x]

    def b_chunk(b):
        return b * (LINE_FIRST_GAP + 1)

    def b0(b):
        product(b_chunk(b), store_line(b))
        hop_send(0, functools.partial(b_up, b), functools.partial(b_down, b), None, None)

    def b_hop(h):
        def go(b):
            hop_send(
                h, functools.partial(b_up, b), functools.partial(b_down, b),
                lambda k: add_blocks(pb.at[b, k], br.at[b, k], (NY, NX)),
                lambda k: add_blocks(pb.at[b, k], bl.at[b, k], (NY, NX)),
            )
        return go

    def b_plane(b):
        @pl.when(has_down)
        def _():
            b_up(b, z).wait_recv()
            add_blocks(pb.at[b, z], br.at[b, z], (NY, NX))

        @pl.when(has_up)
        def _():
            b_down(b, z).wait_recv()
            add_blocks(pb.at[b, z], bl.at[b, z], (NY, NX))

        b_y(b).start()

    def b_second(b):
        b_y(b).wait_recv()
        add_blocks(pb.at[b, z, y], by.at[b], (NX,))
        b_x(b).start()

    def b_last(b):
        b_x(b).wait_recv()
        cols = pl.ds(pl.multiple_of(b_chunk(b) * width, width), width)
        out_ref[:, cols] = pb[b, z, y, x] + bx[b]

    hops = nz - 1
    a_stages = [a0, a1, a2] + [a_hop(h) for h in range(1, hops)] + [a_last]
    b_stages = [b0] + [b_hop(h) for h in range(1, hops)] + [b_plane, b_second, b_last]
    a_at = PLANE_FIRST_STAGES
    b_at = LINE_FIRST_STAGES
    n_steps = max(n_pairs + a_at[-1], (n_line - 1) * LINE_FIRST_GAP + b_at[-1] + 1, 2 * n_tiles)

    def step(t, carry):
        def run_b(j):
            s = t - b_at[j]

            @pl.when((s >= 0) & (lax.rem(s, LINE_FIRST_GAP) == 0) & (lax.div(s, LINE_FIRST_GAP) < n_line))
            def _():
                b_stages[j](lax.div(s, LINE_FIRST_GAP))

        def run_a(j):
            s = t - a_at[j]

            @pl.when((s >= 0) & (s < n_pairs))
            def _():
                a_stages[j](s)

        run_b(0)
        run_a(0)

        @pl.when(t < 2 * n_tiles)
        def _():
            tile(t)

        for j in range(1, len(a_stages)):
            run_a(j)
        for j in range(1, len(b_stages)):
            run_b(j)
        return carry

    lax.fori_loop(0, n_steps, step, 0)

    def drain(p, carry):
        for c in (first_x, first_y, second_y, second_x):
            c(p).wait_send()
        for k in range(nz):
            @pl.when(k > z)
            def _():
                line_up(p, k).wait_send()

            @pl.when(k < z)
            def _():
                line_down(p, k).wait_send()
        return carry

    lax.fori_loop(0, n_pairs, drain, 0)

    def drain_b(b, carry):
        b_y(b).wait_send()
        b_x(b).wait_send()
        for k in range(nz):
            @pl.when(k > z)
            def _():
                b_up(b, k).wait_send()

            @pl.when(k < z)
            def _():
                b_down(b, k).wait_send()
        return carry

    lax.fori_loop(0, n_line, drain_b, 0)
    for i in range(max(n_tiles - 2, 0), n_tiles):
        tin_send(i).wait_send()
        tdown_send(i).wait_send()

    for c in total_copies(n_tiles - 1):
        c.wait()


def exchange(d_in, hidden, w_flat, x_all, dy_all, n_dp, n_rep):
    rows, two_h = d_in.shape
    width = w_flat.shape[0]
    nz = n_dp // (NY * NX)
    share = rows // n_dp
    n_chunks = width // (2 * LANES)
    n_line = n_chunks // LINE_FIRST_SHARE
    n_pairs = n_chunks - n_line
    part = width // n_rep
    d_tile = 256
    n_tiles = part // d_tile
    dims = (nz, n_pairs, n_line, share, d_tile, n_tiles)
    f32 = jnp.float32
    dma = pltpu.SemaphoreType.DMA
    wide = 2 * LANES
    return pl.pallas_call(
        functools.partial(exchange_kernel, dims),
        out_shape=(
            jax.ShapeDtypeStruct((share, width), f32),
            jax.ShapeDtypeStruct((3, part, two_h // 2), f32),
            jax.ShapeDtypeStruct((part, two_h), f32),
            jax.ShapeDtypeStruct((part, two_h // 2), f32),
        ),
        in_specs=[pl.BlockSpec(memory_space=pltpu.VMEM)] * 2 + [pl.BlockSpec(memory_space=pl.ANY)] * 3,
        out_specs=(
            pl.BlockSpec(memory_space=pltpu.VMEM),
            pl.BlockSpec(memory_space=pl.ANY),
            pl.BlockSpec(memory_space=pl.ANY),
            pl.BlockSpec(memory_space=pl.ANY),
        ),
        scratch_shapes=[
            pltpu.VMEM((n_pairs, 2, nz, NY, NX, share, LANES), f32),
            pltpu.VMEM((n_pairs, 2, nz, 2, share, LANES), f32),
            pltpu.VMEM((n_pairs, 2, nz, share, LANES), f32),
            pltpu.VMEM((n_pairs, nz, 2, share, LANES), f32),
            pltpu.VMEM((n_pairs, nz, 2, share, LANES), f32),
            pltpu.VMEM((n_line, nz, NY, NX, share, wide), f32),
            pltpu.VMEM((n_line, nz, NY, NX, share, wide), f32),
            pltpu.VMEM((n_line, nz, NY, NX, share, wide), f32),
            pltpu.VMEM((n_line, share, wide), f32),
            pltpu.VMEM((n_line, NX, share, wide), f32),
            pltpu.VMEM((2, wide, two_h), jnp.bfloat16),
            pltpu.VMEM((2, rows, d_tile), jnp.bfloat16),
            pltpu.VMEM((2, d_tile, two_h), f32),
            pltpu.VMEM((2, d_tile, two_h // 2), f32),
            pltpu.VMEM((d_tile, two_h), f32),
            pltpu.VMEM((d_tile, two_h // 2), f32),
            dma((n_pairs, 2)), dma((n_pairs, 2)), dma((n_pairs, 2)), dma((n_pairs, 2)),
            dma((n_pairs, nz)), dma((n_pairs, nz)), dma((n_pairs, nz)), dma((n_pairs, nz)),
            dma((n_line, nz)), dma((n_line, nz)), dma((n_line, nz)), dma((n_line, nz)),
            dma((n_line,)), dma((n_line,)), dma((n_line,)), dma((n_line,)),
            dma((2,)), dma((2,)), dma((2,)), dma((n_tiles,)), dma((2,)), dma((n_tiles,)), dma((2,)), dma((3,)),
        ],
        compiler_params=pltpu.CompilerParams(
            collective_id=0, has_side_effects=True, vmem_limit_bytes=62 * 2**20
        ),
        cost_estimate=pl.CostEstimate(
            flops=5 * rows * width * two_h // 2, bytes_accessed=8 * width * two_h, transcendentals=0
        ),
    )(d_in, hidden, w_flat, x_all, dy_all)[:2]


def unit_tiles(hidden_units):
    starts = range(0, hidden_units, UNIT_TILE)
    return [(u, min(UNIT_TILE, hidden_units - u)) for u in starts]


def units_kernel(tiles_per_seq, lens_ref, x_ref, dy_ref, w_ref, wd_ref, din_ref, hid_ref, wv, wdv, sems):
    m = pl.program_id(0)
    hidden_units = wd_ref.shape[0]
    pieces = unit_tiles(hidden_units)

    def copies(j):
        u, n = pieces[j]
        return (
            pltpu.make_async_copy(w_ref.at[:, pl.ds(u, n)], wv.at[:, pl.ds(u, n)], sems.at[3 * j]),
            pltpu.make_async_copy(
                w_ref.at[:, pl.ds(hidden_units + u, n)], wv.at[:, pl.ds(hidden_units + u, n)], sems.at[3 * j + 1]
            ),
            pltpu.make_async_copy(wd_ref.at[pl.ds(u, n)], wdv.at[pl.ds(u, n)], sems.at[3 * j + 2]),
        )

    @pl.when(m == 0)
    def _():
        for j in range(len(pieces)):
            for c in copies(j):
                c.start()

    seq = m // tiles_per_seq
    live = lens_ref[seq] - lax.rem(m, tiles_per_seq) * x_ref.shape[0]

    for j, (u, n) in enumerate(pieces):
        @pl.when(m == 0)
        def _():
            for c in copies(j):
                c.wait()

        lo = slice(u, u + n)
        hi = slice(hidden_units + u, hidden_units + u + n)

        @pl.when(live > 0)
        def _():
            gate = jnp.dot(x_ref[...], wv[:, lo], preferred_element_type=jnp.float32)
            upward = jnp.dot(x_ref[...], wv[:, hi], preferred_element_type=jnp.float32)
            d_hidden = lax.dot_general(
                dy_ref[...], wdv[lo, :], (((1,), (1,)), ((), ())), preferred_element_type=jnp.float32
            )
            alive = lax.broadcasted_iota(jnp.int32, gate.shape, 0) < live
            d_hidden = jnp.where(alive, d_hidden, 0.0)
            sigmoid_gate = jax.nn.sigmoid(gate)
            activated = gate * sigmoid_gate
            hid_ref[:, lo] = jnp.where(alive, activated * upward, 0.0).astype(jnp.bfloat16)
            d_gate = d_hidden * upward * sigmoid_gate * (1.0 + gate * (1.0 - sigmoid_gate))
            din_ref[:, lo] = d_gate.astype(jnp.bfloat16)
            din_ref[:, hi] = (d_hidden * activated).astype(jnp.bfloat16)

    @pl.when(live <= 0)
    def _():
        hid_ref[...] = jnp.zeros_like(hid_ref)
        din_ref[...] = jnp.zeros_like(din_ref)


def unit_grads(lens, x_all, dy_all, w_flat, w_down):
    rows, width = x_all.shape
    hidden_units = w_down.shape[0]
    tiles_per_seq = rows // lens.shape[0] // ROW_TILE
    n_sems = 3 * len(unit_tiles(hidden_units))
    row_block = lambda n: pl.BlockSpec((ROW_TILE, n), lambda m, lens: (m, 0))
    return pl.pallas_call(
        functools.partial(units_kernel, tiles_per_seq),
        out_shape=(
            jax.ShapeDtypeStruct((rows, 2 * hidden_units), jnp.bfloat16),
            jax.ShapeDtypeStruct((rows, hidden_units), jnp.bfloat16),
        ),
        grid_spec=pltpu.PrefetchScalarGridSpec(
            num_scalar_prefetch=1,
            grid=(rows // ROW_TILE,),
            in_specs=[row_block(width), row_block(width)] + [pl.BlockSpec(memory_space=pl.ANY)] * 2,
            out_specs=(row_block(2 * hidden_units), row_block(hidden_units)),
            scratch_shapes=[
                pltpu.VMEM((width, 2 * hidden_units), jnp.bfloat16),
                pltpu.VMEM((hidden_units, width), jnp.bfloat16),
                pltpu.SemaphoreType.DMA((n_sems,)),
            ],
        ),
        compiler_params=pltpu.CompilerParams(vmem_limit_bytes=60 * 2**20),
        cost_estimate=pl.CostEstimate(
            flops=6 * rows * width * hidden_units, bytes_accessed=6 * width * hidden_units, transcendentals=0
        ),
    )(lens, x_all, dy_all, w_flat, w_down)


def copy_tiles(src_ref, dst_ref):
    dst_ref[...] = src_ref[...]


def move_out(total, tile=256):
    planes, part, hidden_units = total.shape
    block = pl.BlockSpec((planes, tile, hidden_units), lambda i: (0, i, 0))
    return pl.pallas_call(
        copy_tiles,
        out_shape=jax.ShapeDtypeStruct(total.shape, total.dtype),
        grid=(part // tile,),
        in_specs=[block],
        out_specs=block,
        compiler_params=pltpu.CompilerParams(vmem_limit_bytes=40 * 2**20),
        cost_estimate=pl.CostEstimate(flops=0, bytes_accessed=8 * total.size, transcendentals=0),
    )(total)


def cube_code(index, bits):
    if bits < 2:
        return index
    return index ^ ((index >> 1) & (1 << (bits - 2)))


def bit_slice(blocks, axis, value):
    return lax.index_in_dim(blocks, value, axis, keepdims=False)


def copy_block(owners_ref, src_ref, dst_ref):
    dst_ref[...] = src_ref[...]


def reorder(owners, d_in, share):
    n_dp = owners.shape[0]
    width = d_in.shape[1]
    return pl.pallas_call(
        copy_block,
        out_shape=jax.ShapeDtypeStruct(d_in.shape, d_in.dtype),
        grid_spec=pltpu.PrefetchScalarGridSpec(
            num_scalar_prefetch=1,
            grid=(n_dp,),
            in_specs=[pl.BlockSpec((share, width), lambda i, owners: (owners[i], 0))],
            out_specs=pl.BlockSpec((share, width), lambda i, owners: (i, 0)),
        ),
        cost_estimate=pl.CostEstimate(
            flops=0, bytes_accessed=4 * d_in.size, transcendentals=0
        ),
        compiler_params=pltpu.CompilerParams(vmem_limit_bytes=8 * 2**20),
    )(owners, d_in)


def by_permutes(n_dp, n_rep, tokens, cotangent, lengths, w_in, w_down):
    rows = tokens.shape[1]
    width = tokens.shape[2]
    seqs = lengths.shape[1]
    slots = rows // seqs
    hidden_units = w_down.shape[0]
    bits = n_dp.bit_length() - 1
    share = rows // n_dp
    position = jnp.arange(rows)
    owner_seq = (position // slots)[:, None] == jnp.arange(seqs)[None, :]
    limit = jnp.sum(jnp.where(owner_seq, lengths[0][None, :], 0), axis=1)
    is_alive = position % slots < limit
    zero_value = jnp.zeros((), jnp.bfloat16)
    live_x = jnp.where(is_alive[:, None], tokens[0], zero_value)
    live_dy = jnp.where(is_alive[:, None], cotangent[0], zero_value)
    w_flat = lax.optimization_barrier(w_in.reshape(width, 2 * hidden_units))
    gate_up = jnp.dot(live_x, w_flat, preferred_element_type=jnp.float32)
    gate = gate_up[:, :hidden_units]
    upward = gate_up[:, hidden_units:]
    sigmoid_gate = jax.nn.sigmoid(gate)
    activated = gate * sigmoid_gate
    hidden = (activated * upward).astype(jnp.bfloat16)
    d_hidden = lax.dot_general(
        live_dy, w_down, (((1,), (1,)), ((), ())), preferred_element_type=jnp.float32
    )
    d_gate = d_hidden * upward * sigmoid_gate * (1.0 + gate * (1.0 - sigmoid_gate))
    d_up = d_hidden * activated
    d_in = jnp.concatenate([d_gate, d_up], axis=1).astype(jnp.bfloat16)

    me = lax.axis_index("dp")
    my_code = cube_code(me, bits)
    owners = cube_code(my_code ^ jnp.arange(n_dp, dtype=jnp.int32), bits)
    blocks = reorder(owners, d_in, share)
    blocks = blocks.reshape((2,) * bits + (share, 2 * hidden_units))

    n_chunks = bits * COPIES_PER_ORDER
    while width % n_chunks:
        n_chunks -= 1
    columns = width // n_chunks
    flows = []
    for chunk in range(n_chunks):
        order = [(chunk + step) % bits for step in range(bits)]
        weights = lax.slice_in_dim(w_flat, chunk * columns, (chunk + 1) * columns, axis=0)

        def product(part, weights=weights):
            return lax.dot_general(
                part, weights, (((part.ndim - 1,), (1,)), ((), ())), preferred_element_type=jnp.float32
            )

        axis = bits - 1 - order[0]
        sent = product(bit_slice(blocks, axis, 1))
        kept = product(bit_slice(blocks, axis, 0))
        flows.append((order, sent, kept))

    def partner_pairs(bit):
        return [(d, cube_code(cube_code(d, bits) ^ (1 << bit), bits)) for d in range(n_dp)]

    part = width // n_rep
    rep = lax.axis_index("rep")

    def gradients(owner, after):
        x_all, dy_all, d_all, h_all, _ = lax.optimization_barrier((live_x, live_dy, d_in, hidden, after))
        x_part = lax.dynamic_slice_in_dim(x_all, owner * part, part, 1)
        dy_part = lax.dynamic_slice_in_dim(dy_all, owner * part, part, 1)
        pairs = (
            (x_part, d_all[:, :hidden_units]),
            (x_part, d_all[:, hidden_units:]),
            (dy_part, h_all),
        )
        return lax.optimization_barrier(
            tuple(
                lax.dot_general(
                    rows_of, units, (((0,), (0,)), ((), ())), preferred_element_type=jnp.float32
                )
                for rows_of, units in pairs
            )
        )

    first_sent = tuple(sent for _, sent, _ in flows)
    totals = [[], [], []]
    for shift in range(1, n_rep):
        ring = [(r, (r + shift) % n_rep) for r in range(n_rep)]
        for kind, grad in enumerate(gradients((rep + shift) % n_rep, first_sent)):
            totals[kind].append(lax.ppermute(grad, "rep", ring))

    results = [None] * n_chunks
    state = {}
    for chunk, (order, sent, kept) in enumerate(flows):
        state[chunk] = (sent, kept, sorted(order, reverse=True))
    shared = None
    for step in range(bits):
        if step == 1:
            own = gradients(rep, tuple(state[chunk][0] for chunk in range(min(bits, n_chunks))))
            for kind in range(3):
                totals[kind].append(own[kind])
            shared = jnp.stack([sum(terms[1:], terms[0]) for terms in totals], axis=1) * GRAD_SCALE
        for chunk in range(n_chunks):
            order = flows[chunk][0]
            sent, kept, left = state[chunk]
            if step == bits - 1 and shared is not None and chunk >= n_chunks // 2:
                sent, _ = lax.optimization_barrier((sent, shared))
            got = lax.ppermute(sent, "dp", partner_pairs(order[step]))
            left = [b for b in left if b != order[step]]
            if step == bits - 1:
                results[chunk] = kept + got
            else:
                axis = left.index(order[step + 1])
                sent = bit_slice(kept, axis, 1) + bit_slice(got, axis, 1)
                kept = bit_slice(kept, axis, 0) + bit_slice(got, axis, 0)
                state[chunk] = (sent, kept, left)
    shard = jnp.concatenate(results, axis=1)
    return (shard[None], shared)


def by_kernels(n_dp, n_rep, tokens, cotangent, lengths, w_in, w_down):
    width = tokens.shape[2]
    hidden_units = w_down.shape[0]
    w_flat = lax.optimization_barrier(w_in.reshape(width, 2 * hidden_units))
    d_in, hidden = unit_grads(lengths[0], tokens[0], cotangent[0], w_flat, w_down)
    shard, total = exchange(d_in, hidden, w_flat, tokens[0], cotangent[0], n_dp, n_rep)
    return (shard[None], move_out(total).transpose(1, 0, 2))


def fits_kernels(n_dp, n_rep, rows, seqs, width, hidden_units):
    return (
        n_rep == 2
        and n_dp == LINE * NY * NX
        and rows % (16 * n_dp) == 0
        and rows % (seqs * ROW_TILE) == 0
        and width % (n_rep * 256) == 0
        and hidden_units % (2 * LANES) in (0, LANES)
    )


def solution(mesh):
    n_dp = mesh.shape["dp"]
    n_rep = mesh.shape["rep"]

    def body(*args):
        tokens, _, _, _, w_down = args
        fast = fits_kernels(n_dp, n_rep, tokens.shape[1], args[2].shape[1], tokens.shape[2], w_down.shape[0])
        return (by_kernels if fast else by_permutes)(n_dp, n_rep, *args)

    in_specs = (
        P("rep", None, None),
        P("rep", None, None),
        P("rep", None),
        P(None, None, "dp"),
        P("dp", None),
    )
    out_specs = (P("rep", "dp", None), P("rep", None, "dp"))
    return jax.shard_map(
        body, mesh=mesh, in_specs=in_specs, out_specs=out_specs, check_vma=False
    )
```

```python
import functools
import jax
import jax.numpy as jnp
from jax import lax
from jax.experimental import pallas as pl
from jax.experimental.pallas import tpu as pltpu

from jax.sharding import PartitionSpec as P

GRAD_SCALE = 0.03125
COPIES_PER_ORDER = 2
MESH = pl.DeviceIdType.MESH
LINE = 4
NY = 2
NX = 2
LANES = 128
PLANE_FIRST_STAGES = (0, 3, 6, 9, 11, 13)
LINE_FIRST_STAGES = (0, 4, 7, 13, 15, 17)
ROW_TILE = 256
UNIT_TILE = 256
LINE_FIRST_GAP = 2
LINE_FIRST_SHARE = 4


def add_blocks(dst, src, lead):
    count = 1
    for n in lead:
        count *= n

    def body(i, carry):
        idx = []
        for n in reversed(lead):
            idx.append(lax.rem(i, n))
            i = i // n
        idx = tuple(reversed(idx))
        dst[idx] = dst[idx] + src[idx]
        return carry

    if count == 1:
        dst[...] = dst[...] + src[...]
    else:
        lax.fori_loop(0, count, body, 0)


def exchange_kernel(
    dims, d_in, hidden, w_ref, x_ref, dy_ref, out_ref, total, g_in, g_down,
    pa, rs1, rs2, zr, zl, pb, br, bl, bx, by, wbuf, xbuf, tin, tdown, gin, gdown,
    s1s, s1r, s2s, s2r, zrs, zrr, zls, zlr, brs, brr, bls, blr, bxs, bxr, bys, byr,
    wsem, xsem, tis, tir, tds, tdr, gsem, osem,
):
    nz, n_pairs, n_line, share, d_tile, n_tiles = dims
    d = lax.axis_index("dp")
    rep = lax.axis_index("rep")
    z, y, x = d // (NY * NX), lax.rem(d // NX, NY), lax.rem(d, NX)
    px = d + 1 - 2 * x
    py = d + NX * (1 - 2 * y)
    up, down = d + NY * NX, d - NY * NX
    has_up, has_down = z < nz - 1, z > 0
    other = 1 - rep
    width = 2 * LANES
    rows = d_in.shape[0]
    m_tile = NY * NX * share
    part = n_tiles * d_tile

    barrier = pltpu.get_barrier_semaphore()
    for peer in (px, py):
        pl.semaphore_signal(barrier, inc=1, device_id=(peer, rep), device_id_type=MESH)
    pl.semaphore_signal(barrier, inc=1, device_id=(d, other), device_id_type=MESH)

    @pl.when(has_up)
    def _():
        pl.semaphore_signal(barrier, inc=1, device_id=(up, rep), device_id_type=MESH)

    @pl.when(has_down)
    def _():
        pl.semaphore_signal(barrier, inc=1, device_id=(down, rep), device_id_type=MESH)

    pl.semaphore_wait(barrier, 3 + has_up.astype(jnp.int32) + has_down.astype(jnp.int32))

    def remote(src, dst, ssem, rsem, dev, core=None):
        return pltpu.make_async_remote_copy(
            src_ref=src, dst_ref=dst, send_sem=ssem, recv_sem=rsem,
            device_id=(dev, rep if core is None else core), device_id_type=MESH,
        )

    def first_x(p):
        return remote(pa.at[p, 0, :, :, 1 - x], rs1.at[p, 0], s1s.at[p, 0], s1r.at[p, 0], px)

    def first_y(p):
        return remote(pa.at[p, 1, :, 1 - y], rs1.at[p, 1], s1s.at[p, 1], s1r.at[p, 1], py)

    def second_y(p):
        return remote(pa.at[p, 0, :, 1 - y, x], rs2.at[p, 0], s2s.at[p, 0], s2r.at[p, 0], py)

    def second_x(p):
        return remote(pa.at[p, 1, :, y, 1 - x], rs2.at[p, 1], s2s.at[p, 1], s2r.at[p, 1], px)

    def line_up(p, k):
        return remote(pa.at[p, :, k, y, x], zr.at[p, k], zrs.at[p, k], zrr.at[p, k], up)

    def line_down(p, k):
        return remote(pa.at[p, :, k, y, x], zl.at[p, k], zls.at[p, k], zlr.at[p, k], down)

    def b_up(b, k):
        return remote(pb.at[b, k], br.at[b, k], brs.at[b, k], brr.at[b, k], up)

    def b_down(b, k):
        return remote(pb.at[b, k], bl.at[b, k], bls.at[b, k], blr.at[b, k], down)

    def b_y(b):
        return remote(pb.at[b, z, 1 - y], by.at[b], bys.at[b], byr.at[b], py)

    def b_x(b):
        return remote(pb.at[b, z, y, 1 - x], bx.at[b], bxs.at[b], bxr.at[b], px)

    def w_copy(c):
        slot = lax.rem(c, 2)
        return pltpu.make_async_copy(w_ref.at[pl.ds(c * width, width)], wbuf.at[slot], wsem.at[slot])

    n_chunks = n_pairs + n_line
    w_copy(0).start()

    def product(c, store):
        w_copy(c).wait()

        @pl.when(c + 1 < n_chunks)
        def _():
            w_copy(c + 1).start()

        slot = lax.rem(c, 2)

        def body(k, carry):
            val = lax.dot_general(
                d_in[pl.ds(pl.multiple_of(k * m_tile, m_tile), m_tile), :], wbuf[slot],
                (((1,), (1,)), ((), ())), preferred_element_type=jnp.float32,
            )
            store(k, val)
            return carry

        lax.fori_loop(0, nz, body, 0)

    def store_pair(p):
        def store(k, val):
            val = val.reshape(NY, NX, share, width)
            pa[p, 0, k] = val[..., :LANES]
            pa[p, 1, k] = val[..., LANES:]
        return store

    def store_line(b):
        def store(k, val):
            pb[b, k] = val.reshape(NY, NX, share, width)
        return store

    def x_copy(i, src, s):
        core = jnp.where(i < n_tiles, other, rep)
        off = pl.multiple_of(core * part + lax.rem(i, n_tiles) * d_tile, d_tile)
        return pltpu.make_async_copy(src.at[:, pl.ds(off, d_tile)], xbuf.at[s], xsem.at[s])

    def tin_send(i):
        slot = lax.rem(i, 2)
        return remote(tin.at[slot], g_in.at[pl.ds(i * d_tile, d_tile)], tis.at[slot], tir.at[i], d, other)

    def tdown_send(i):
        slot = lax.rem(i, 2)
        return remote(tdown.at[slot], g_down.at[pl.ds(i * d_tile, d_tile)], tds.at[slot], tdr.at[i], d, other)

    def got_copies(i):
        at = pl.ds(i * d_tile, d_tile)
        return (
            pltpu.make_async_copy(g_in.at[at], gin, gsem.at[0]),
            pltpu.make_async_copy(g_down.at[at], gdown, gsem.at[1]),
        )

    def total_copies(i):
        at = pl.ds(i * d_tile, d_tile)
        units = gdown.shape[1]
        return (
            pltpu.make_async_copy(gin.at[:, pl.ds(0, units)], total.at[0, at], osem.at[0]),
            pltpu.make_async_copy(gin.at[:, pl.ds(units, units)], total.at[1, at], osem.at[1]),
            pltpu.make_async_copy(gdown, total.at[2, at], osem.at[2]),
        )

    def columns(store):
        lhs = xbuf[0].T

        def body(n, carry):
            cols = pl.ds(pl.multiple_of(n * width, width), width)
            store(cols, jnp.dot(lhs, d_in[:, cols], preferred_element_type=jnp.float32))
            return carry

        lax.fori_loop(0, d_in.shape[1] // width, body, 0)
        return jnp.dot(xbuf[1].T, hidden[...], preferred_element_type=jnp.float32)

    def tile(i):
        x_copy(i, x_ref, 0).wait()
        x_copy(i, dy_ref, 1).wait()

        @pl.when(i < n_tiles)
        def _():
            slot = lax.rem(i, 2)

            @pl.when(i >= 2)
            def _():
                tin_send(i - 2).wait_send()
                tdown_send(i - 2).wait_send()

            def store(cols, val):
                tin[slot, :, cols] = val

            tdown[slot] = columns(store)
            tin_send(i).start()
            tdown_send(i).start()

        @pl.when(i >= n_tiles)
        def _():
            k = i - n_tiles

            @pl.when(k >= 1)
            def _():
                for c in total_copies(k - 1):
                    c.wait()

            tin_send(k).wait_recv()
            tdown_send(k).wait_recv()
            for c in got_copies(k):
                c.start()
            for c in got_copies(k):
                c.wait()

            def store(cols, val):
                gin[:, cols] = (gin[:, cols] + val) * GRAD_SCALE

            gdown[...] = (gdown[...] + columns(store)) * GRAD_SCALE
            for c in total_copies(k):
                c.start()

        @pl.when(i + 1 < 2 * n_tiles)
        def _():
            x_copy(i + 1, x_ref, 0).start()
            x_copy(i + 1, dy_ref, 1).start()

    x_copy(0, x_ref, 0).start()
    x_copy(0, dy_ref, 1).start()

    def a0(p):
        product(p + jnp.minimum(lax.div(p, LINE_FIRST_GAP) + 1, n_line), store_pair(p))
        first_x(p).start()
        first_y(p).start()

    def a1(p):
        first_x(p).wait_recv()
        add_blocks(pa.at[p, 0, :, 1 - y, x], rs1.at[p, 0, :, 1 - y], (nz,))
        second_y(p).start()
        first_y(p).wait_recv()
        add_blocks(pa.at[p, 1, :, y, 1 - x], rs1.at[p, 1, :, 1 - x], (nz,))
        second_x(p).start()
        add_blocks(pa.at[p, 0, :, y, x], rs1.at[p, 0, :, y], (nz,))
        add_blocks(pa.at[p, 1, :, y, x], rs1.at[p, 1, :, x], (nz,))

    def a2(p):
        second_y(p).wait_recv()
        add_blocks(pa.at[p, 0, :, y, x], rs2.at[p, 0], (nz,))
        second_x(p).wait_recv()
        add_blocks(pa.at[p, 1, :, y, x], rs2.at[p, 1], (nz,))
        hop_send(0, functools.partial(line_up, p), functools.partial(line_down, p), None, None)

    def hop_send(h, cup, cdown, add_up, add_down):
        @pl.when(z == h)
        def _():
            for k in range(nz - 1, h, -1):
                if h:
                    cup(k).wait_recv()
                    add_up(k)
                cup(k).start()

        @pl.when(z == nz - 1 - h)
        def _():
            for k in range(0, nz - 1 - h):
                if h:
                    cdown(k).wait_recv()
                    add_down(k)
                cdown(k).start()

    def a_hop(h):
        def go(p):
            hop_send(
                h, functools.partial(line_up, p), functools.partial(line_down, p),
                lambda k: add_blocks(pa.at[p, :, k, y, x], zr.at[p, k], (2,)),
                lambda k: add_blocks(pa.at[p, :, k, y, x], zl.at[p, k], (2,)),
            )
        return go

    def a_last(p):
        @pl.when(has_down)
        def _():
            line_up(p, z).wait_recv()
            add_blocks(pa.at[p, :, z, y, x], zr.at[p, z], (2,))

        @pl.when(has_up)
        def _():
            line_down(p, z).wait_recv()
            add_blocks(pa.at[p, :, z, y, x], zl.at[p, z], (2,))

        c = p + jnp.minimum(lax.div(p, LINE_FIRST_GAP) + 1, n_line)
        for u in range(2):
            cols = pl.ds(pl.multiple_of(c * width + u * LANES, LANES), LANES)
            out_ref[:, cols] = pa[p, u, z, y, x]

    def b_chunk(b):
        return b * (LINE_FIRST_GAP + 1)

    def b0(b):
        product(b_chunk(b), store_line(b))
        hop_send(0, functools.partial(b_up, b), functools.partial(b_down, b), None, None)

    def b_hop(h):
        def go(b):
            hop_send(
                h, functools.partial(b_up, b), functools.partial(b_down, b),
                lambda k: add_blocks(pb.at[b, k], br.at[b, k], (NY, NX)),
                lambda k: add_blocks(pb.at[b, k], bl.at[b, k], (NY, NX)),
            )
        return go

    def b_plane(b):
        @pl.when(has_down)
        def _():
            b_up(b, z).wait_recv()
            add_blocks(pb.at[b, z], br.at[b, z], (NY, NX))

        @pl.when(has_up)
        def _():
            b_down(b, z).wait_recv()
            add_blocks(pb.at[b, z], bl.at[b, z], (NY, NX))

        b_y(b).start()

    def b_second(b):
        b_y(b).wait_recv()
        add_blocks(pb.at[b, z, y], by.at[b], (NX,))
        b_x(b).start()

    def b_last(b):
        b_x(b).wait_recv()
        cols = pl.ds(pl.multiple_of(b_chunk(b) * width, width), width)
        out_ref[:, cols] = pb[b, z, y, x] + bx[b]

    hops = nz - 1
    a_stages = [a0, a1, a2] + [a_hop(h) for h in range(1, hops)] + [a_last]
    b_stages = [b0] + [b_hop(h) for h in range(1, hops)] + [b_plane, b_second, b_last]
    a_at = PLANE_FIRST_STAGES
    b_at = LINE_FIRST_STAGES
    n_steps = max(n_pairs + a_at[-1], (n_line - 1) * LINE_FIRST_GAP + b_at[-1] + 1, 2 * n_tiles)

    def step(t, carry):
        def run_b(j):
            s = t - b_at[j]

            @pl.when((s >= 0) & (lax.rem(s, LINE_FIRST_GAP) == 0) & (lax.div(s, LINE_FIRST_GAP) < n_line))
            def _():
                b_stages[j](lax.div(s, LINE_FIRST_GAP))

        def run_a(j):
            s = t - a_at[j]

            @pl.when((s >= 0) & (s < n_pairs))
            def _():
                a_stages[j](s)

        run_b(0)
        run_a(0)

        @pl.when(t < 2 * n_tiles)
        def _():
            tile(t)

        for j in range(1, len(a_stages)):
            run_a(j)
        for j in range(1, len(b_stages)):
            run_b(j)
        return carry

    lax.fori_loop(0, n_steps, step, 0)

    def drain(p, carry):
        for c in (first_x, first_y, second_y, second_x):
            c(p).wait_send()
        for k in range(nz):
            @pl.when(k > z)
            def _():
                line_up(p, k).wait_send()

            @pl.when(k < z)
            def _():
                line_down(p, k).wait_send()
        return carry

    lax.fori_loop(0, n_pairs, drain, 0)

    def drain_b(b, carry):
        b_y(b).wait_send()
        b_x(b).wait_send()
        for k in range(nz):
            @pl.when(k > z)
            def _():
                b_up(b, k).wait_send()

            @pl.when(k < z)
            def _():
                b_down(b, k).wait_send()
        return carry

    lax.fori_loop(0, n_line, drain_b, 0)
    for i in range(max(n_tiles - 2, 0), n_tiles):
        tin_send(i).wait_send()
        tdown_send(i).wait_send()

    for c in total_copies(n_tiles - 1):
        c.wait()


def exchange(d_in, hidden, w_flat, x_all, dy_all, n_dp, n_rep):
    rows, two_h = d_in.shape
    width = w_flat.shape[0]
    nz = n_dp // (NY * NX)
    share = rows // n_dp
    n_chunks = width // (2 * LANES)
    n_line = n_chunks // LINE_FIRST_SHARE
    n_pairs = n_chunks - n_line
    part = width // n_rep
    d_tile = 256
    n_tiles = part // d_tile
    dims = (nz, n_pairs, n_line, share, d_tile, n_tiles)
    f32 = jnp.float32
    dma = pltpu.SemaphoreType.DMA
    wide = 2 * LANES
    return pl.pallas_call(
        functools.partial(exchange_kernel, dims),
        out_shape=(
            jax.ShapeDtypeStruct((share, width), f32),
            jax.ShapeDtypeStruct((3, part, two_h // 2), f32),
            jax.ShapeDtypeStruct((part, two_h), f32),
            jax.ShapeDtypeStruct((part, two_h // 2), f32),
        ),
        in_specs=[pl.BlockSpec(memory_space=pltpu.VMEM)] * 2 + [pl.BlockSpec(memory_space=pl.ANY)] * 3,
        out_specs=(
            pl.BlockSpec(memory_space=pltpu.VMEM),
            pl.BlockSpec(memory_space=pl.ANY),
            pl.BlockSpec(memory_space=pl.ANY),
            pl.BlockSpec(memory_space=pl.ANY),
        ),
        scratch_shapes=[
            pltpu.VMEM((n_pairs, 2, nz, NY, NX, share, LANES), f32),
            pltpu.VMEM((n_pairs, 2, nz, 2, share, LANES), f32),
            pltpu.VMEM((n_pairs, 2, nz, share, LANES), f32),
            pltpu.VMEM((n_pairs, nz, 2, share, LANES), f32),
            pltpu.VMEM((n_pairs, nz, 2, share, LANES), f32),
            pltpu.VMEM((n_line, nz, NY, NX, share, wide), f32),
            pltpu.VMEM((n_line, nz, NY, NX, share, wide), f32),
            pltpu.VMEM((n_line, nz, NY, NX, share, wide), f32),
            pltpu.VMEM((n_line, share, wide), f32),
            pltpu.VMEM((n_line, NX, share, wide), f32),
            pltpu.VMEM((2, wide, two_h), jnp.bfloat16),
            pltpu.VMEM((2, rows, d_tile), jnp.bfloat16),
            pltpu.VMEM((2, d_tile, two_h), f32),
            pltpu.VMEM((2, d_tile, two_h // 2), f32),
            pltpu.VMEM((d_tile, two_h), f32),
            pltpu.VMEM((d_tile, two_h // 2), f32),
            dma((n_pairs, 2)), dma((n_pairs, 2)), dma((n_pairs, 2)), dma((n_pairs, 2)),
            dma((n_pairs, nz)), dma((n_pairs, nz)), dma((n_pairs, nz)), dma((n_pairs, nz)),
            dma((n_line, nz)), dma((n_line, nz)), dma((n_line, nz)), dma((n_line, nz)),
            dma((n_line,)), dma((n_line,)), dma((n_line,)), dma((n_line,)),
            dma((2,)), dma((2,)), dma((2,)), dma((n_tiles,)), dma((2,)), dma((n_tiles,)), dma((2,)), dma((3,)),
        ],
        compiler_params=pltpu.CompilerParams(
            collective_id=0, has_side_effects=True, vmem_limit_bytes=62 * 2**20
        ),
        cost_estimate=pl.CostEstimate(
            flops=5 * rows * width * two_h // 2, bytes_accessed=8 * width * two_h, transcendentals=0
        ),
    )(d_in, hidden, w_flat, x_all, dy_all)[:2]


def unit_tiles(hidden_units):
    starts = range(0, hidden_units, UNIT_TILE)
    return [(u, min(UNIT_TILE, hidden_units - u)) for u in starts]


def units_kernel(tiles_per_seq, lens_ref, x_ref, dy_ref, w_ref, wd_ref, din_ref, hid_ref, wv, wdv, sems):
    m = pl.program_id(0)
    hidden_units = wd_ref.shape[0]
    pieces = unit_tiles(hidden_units)

    def copies(j):
        u, n = pieces[j]
        return (
            pltpu.make_async_copy(w_ref.at[:, pl.ds(u, n)], wv.at[:, pl.ds(u, n)], sems.at[3 * j]),
            pltpu.make_async_copy(
                w_ref.at[:, pl.ds(hidden_units + u, n)], wv.at[:, pl.ds(hidden_units + u, n)], sems.at[3 * j + 1]
            ),
            pltpu.make_async_copy(wd_ref.at[pl.ds(u, n)], wdv.at[pl.ds(u, n)], sems.at[3 * j + 2]),
        )

    @pl.when(m == 0)
    def _():
        for j in range(min(2, len(pieces))):
            for c in copies(j):
                c.start()

    seq = m // tiles_per_seq
    live = lens_ref[seq] - lax.rem(m, tiles_per_seq) * x_ref.shape[0]

    for j, (u, n) in enumerate(pieces):
        @pl.when(m == 0)
        def _():
            for c in copies(j):
                c.wait()
            if j + 2 < len(pieces):
                for c in copies(j + 2):
                    c.start()

        lo = slice(u, u + n)
        hi = slice(hidden_units + u, hidden_units + u + n)

        @pl.when(live > 0)
        def _():
            gate = jnp.dot(x_ref[...], wv[:, lo], preferred_element_type=jnp.float32)
            upward = jnp.dot(x_ref[...], wv[:, hi], preferred_element_type=jnp.float32)
            d_hidden = lax.dot_general(
                dy_ref[...], wdv[lo, :], (((1,), (1,)), ((), ())), preferred_element_type=jnp.float32
            )
            alive = lax.broadcasted_iota(jnp.int32, gate.shape, 0) < live
            d_hidden = jnp.where(alive, d_hidden, 0.0)
            sigmoid_gate = jax.nn.sigmoid(gate)
            activated = gate * sigmoid_gate
            hid_ref[:, lo] = jnp.where(alive, activated * upward, 0.0).astype(jnp.bfloat16)
            d_gate = d_hidden * upward * sigmoid_gate * (1.0 + gate * (1.0 - sigmoid_gate))
            din_ref[:, lo] = d_gate.astype(jnp.bfloat16)
            din_ref[:, hi] = (d_hidden * activated).astype(jnp.bfloat16)

    @pl.when(live <= 0)
    def _():
        hid_ref[...] = jnp.zeros_like(hid_ref)
        din_ref[...] = jnp.zeros_like(din_ref)


def unit_grads(lens, x_all, dy_all, w_flat, w_down):
    rows, width = x_all.shape
    hidden_units = w_down.shape[0]
    tiles_per_seq = rows // lens.shape[0] // ROW_TILE
    n_sems = 3 * len(unit_tiles(hidden_units))
    row_block = lambda n: pl.BlockSpec((ROW_TILE, n), lambda m, lens: (m, 0))
    return pl.pallas_call(
        functools.partial(units_kernel, tiles_per_seq),
        out_shape=(
            jax.ShapeDtypeStruct((rows, 2 * hidden_units), jnp.bfloat16),
            jax.ShapeDtypeStruct((rows, hidden_units), jnp.bfloat16),
        ),
        grid_spec=pltpu.PrefetchScalarGridSpec(
            num_scalar_prefetch=1,
            grid=(rows // ROW_TILE,),
            in_specs=[row_block(width), row_block(width)] + [pl.BlockSpec(memory_space=pl.ANY)] * 2,
            out_specs=(row_block(2 * hidden_units), row_block(hidden_units)),
            scratch_shapes=[
                pltpu.VMEM((width, 2 * hidden_units), jnp.bfloat16),
                pltpu.VMEM((hidden_units, width), jnp.bfloat16),
                pltpu.SemaphoreType.DMA((n_sems,)),
            ],
        ),
        compiler_params=pltpu.CompilerParams(vmem_limit_bytes=60 * 2**20),
        cost_estimate=pl.CostEstimate(
            flops=6 * rows * width * hidden_units, bytes_accessed=6 * width * hidden_units, transcendentals=0
        ),
    )(lens, x_all, dy_all, w_flat, w_down)


def copy_tiles(src_ref, dst_ref):
    dst_ref[...] = src_ref[...]


def move_out(total, tile=256):
    planes, part, hidden_units = total.shape
    block = pl.BlockSpec((planes, tile, hidden_units), lambda i: (0, i, 0))
    return pl.pallas_call(
        copy_tiles,
        out_shape=jax.ShapeDtypeStruct(total.shape, total.dtype),
        grid=(part // tile,),
        in_specs=[block],
        out_specs=block,
        compiler_params=pltpu.CompilerParams(vmem_limit_bytes=40 * 2**20),
        cost_estimate=pl.CostEstimate(flops=0, bytes_accessed=8 * total.size, transcendentals=0),
    )(total)


def cube_code(index, bits):
    if bits < 2:
        return index
    return index ^ ((index >> 1) & (1 << (bits - 2)))


def bit_slice(blocks, axis, value):
    return lax.index_in_dim(blocks, value, axis, keepdims=False)


def copy_block(owners_ref, src_ref, dst_ref):
    dst_ref[...] = src_ref[...]


def reorder(owners, d_in, share):
    n_dp = owners.shape[0]
    width = d_in.shape[1]
    return pl.pallas_call(
        copy_block,
        out_shape=jax.ShapeDtypeStruct(d_in.shape, d_in.dtype),
        grid_spec=pltpu.PrefetchScalarGridSpec(
            num_scalar_prefetch=1,
            grid=(n_dp,),
            in_specs=[pl.BlockSpec((share, width), lambda i, owners: (owners[i], 0))],
            out_specs=pl.BlockSpec((share, width), lambda i, owners: (i, 0)),
        ),
        cost_estimate=pl.CostEstimate(
            flops=0, bytes_accessed=4 * d_in.size, transcendentals=0
        ),
        compiler_params=pltpu.CompilerParams(vmem_limit_bytes=8 * 2**20),
    )(owners, d_in)


def by_permutes(n_dp, n_rep, tokens, cotangent, lengths, w_in, w_down):
    rows = tokens.shape[1]
    width = tokens.shape[2]
    seqs = lengths.shape[1]
    slots = rows // seqs
    hidden_units = w_down.shape[0]
    bits = n_dp.bit_length() - 1
    share = rows // n_dp
    position = jnp.arange(rows)
    owner_seq = (position // slots)[:, None] == jnp.arange(seqs)[None, :]
    limit = jnp.sum(jnp.where(owner_seq, lengths[0][None, :], 0), axis=1)
    is_alive = position % slots < limit
    zero_value = jnp.zeros((), jnp.bfloat16)
    live_x = jnp.where(is_alive[:, None], tokens[0], zero_value)
    live_dy = jnp.where(is_alive[:, None], cotangent[0], zero_value)
    w_flat = lax.optimization_barrier(w_in.reshape(width, 2 * hidden_units))
    gate_up = jnp.dot(live_x, w_flat, preferred_element_type=jnp.float32)
    gate = gate_up[:, :hidden_units]
    upward = gate_up[:, hidden_units:]
    sigmoid_gate = jax.nn.sigmoid(gate)
    activated = gate * sigmoid_gate
    hidden = (activated * upward).astype(jnp.bfloat16)
    d_hidden = lax.dot_general(
        live_dy, w_down, (((1,), (1,)), ((), ())), preferred_element_type=jnp.float32
    )
    d_gate = d_hidden * upward * sigmoid_gate * (1.0 + gate * (1.0 - sigmoid_gate))
    d_up = d_hidden * activated
    d_in = jnp.concatenate([d_gate, d_up], axis=1).astype(jnp.bfloat16)

    me = lax.axis_index("dp")
    my_code = cube_code(me, bits)
    owners = cube_code(my_code ^ jnp.arange(n_dp, dtype=jnp.int32), bits)
    blocks = reorder(owners, d_in, share)
    blocks = blocks.reshape((2,) * bits + (share, 2 * hidden_units))

    n_chunks = bits * COPIES_PER_ORDER
    while width % n_chunks:
        n_chunks -= 1
    columns = width // n_chunks
    flows = []
    for chunk in range(n_chunks):
        order = [(chunk + step) % bits for step in range(bits)]
        weights = lax.slice_in_dim(w_flat, chunk * columns, (chunk + 1) * columns, axis=0)

        def product(part, weights=weights):
            return lax.dot_general(
                part, weights, (((part.ndim - 1,), (1,)), ((), ())), preferred_element_type=jnp.float32
            )

        axis = bits - 1 - order[0]
        sent = product(bit_slice(blocks, axis, 1))
        kept = product(bit_slice(blocks, axis, 0))
        flows.append((order, sent, kept))

    def partner_pairs(bit):
        return [(d, cube_code(cube_code(d, bits) ^ (1 << bit), bits)) for d in range(n_dp)]

    part = width // n_rep
    rep = lax.axis_index("rep")

    def gradients(owner, after):
        x_all, dy_all, d_all, h_all, _ = lax.optimization_barrier((live_x, live_dy, d_in, hidden, after))
        x_part = lax.dynamic_slice_in_dim(x_all, owner * part, part, 1)
        dy_part = lax.dynamic_slice_in_dim(dy_all, owner * part, part, 1)
        pairs = (
            (x_part, d_all[:, :hidden_units]),
            (x_part, d_all[:, hidden_units:]),
            (dy_part, h_all),
        )
        return lax.optimization_barrier(
            tuple(
                lax.dot_general(
                    rows_of, units, (((0,), (0,)), ((), ())), preferred_element_type=jnp.float32
                )
                for rows_of, units in pairs
            )
        )

    first_sent = tuple(sent for _, sent, _ in flows)
    totals = [[], [], []]
    for shift in range(1, n_rep):
        ring = [(r, (r + shift) % n_rep) for r in range(n_rep)]
        for kind, grad in enumerate(gradients((rep + shift) % n_rep, first_sent)):
            totals[kind].append(lax.ppermute(grad, "rep", ring))

    results = [None] * n_chunks
    state = {}
    for chunk, (order, sent, kept) in enumerate(flows):
        state[chunk] = (sent, kept, sorted(order, reverse=True))
    shared = None
    for step in range(bits):
        if step == 1:
            own = gradients(rep, tuple(state[chunk][0] for chunk in range(min(bits, n_chunks))))
            for kind in range(3):
                totals[kind].append(own[kind])
            shared = jnp.stack([sum(terms[1:], terms[0]) for terms in totals], axis=1) * GRAD_SCALE
        for chunk in range(n_chunks):
            order = flows[chunk][0]
            sent, kept, left = state[chunk]
            if step == bits - 1 and shared is not None and chunk >= n_chunks // 2:
                sent, _ = lax.optimization_barrier((sent, shared))
            got = lax.ppermute(sent, "dp", partner_pairs(order[step]))
            left = [b for b in left if b != order[step]]
            if step == bits - 1:
                results[chunk] = kept + got
            else:
                axis = left.index(order[step + 1])
                sent = bit_slice(kept, axis, 1) + bit_slice(got, axis, 1)
                kept = bit_slice(kept, axis, 0) + bit_slice(got, axis, 0)
                state[chunk] = (sent, kept, left)
    shard = jnp.concatenate(results, axis=1)
    return (shard[None], shared)


def by_kernels(n_dp, n_rep, tokens, cotangent, lengths, w_in, w_down):
    width = tokens.shape[2]
    hidden_units = w_down.shape[0]
    w_flat = lax.optimization_barrier(w_in.reshape(width, 2 * hidden_units))
    d_in, hidden = unit_grads(lengths[0], tokens[0], cotangent[0], w_flat, w_down)
    shard, total = exchange(d_in, hidden, w_flat, tokens[0], cotangent[0], n_dp, n_rep)
    return (shard[None], move_out(total).transpose(1, 0, 2))


def fits_kernels(n_dp, n_rep, rows, seqs, width, hidden_units):
    return (
        n_rep == 2
        and n_dp == LINE * NY * NX
        and rows % (16 * n_dp) == 0
        and rows % (seqs * ROW_TILE) == 0
        and width % (n_rep * 256) == 0
        and hidden_units % (2 * LANES) in (0, LANES)
    )


def solution(mesh):
    n_dp = mesh.shape["dp"]
    n_rep = mesh.shape["rep"]

    def body(*args):
        tokens, _, _, _, w_down = args
        fast = fits_kernels(n_dp, n_rep, tokens.shape[1], args[2].shape[1], tokens.shape[2], w_down.shape[0])
        return (by_kernels if fast else by_permutes)(n_dp, n_rep, *args)

    in_specs = (
        P("rep", None, None),
        P("rep", None, None),
        P("rep", None),
        P(None, None, "dp"),
        P("dp", None),
    )
    out_specs = (P("rep", "dp", None), P("rep", None, "dp"))
    return jax.shard_map(
        body, mesh=mesh, in_specs=in_specs, out_specs=out_specs, check_vma=False
    )
```
